256 devices in a mesh: nest: 4 (over y), tile: 64 (over z, x, core).
Axes of the slice: x: 4, y: 4, z: 8, core: 2. Of those that a mesh axis runs over, the one named last changes fastest.
Arguments:
- child_fields: float32 [4, 32, 1536, 3072], P('nest', None, 'tile'), may hold values from -18 to 18
- row_weights: float32 [8, 24], replicated
- col_weights: float32 [3072, 1024], replicated
- nest_offsets: int32 [4, 2], replicated, may hold values from 0 to 1023, as said below
- priority: int32 [1024, 1024], P('tile', 'nest'), may hold values from -1 to 3, as said below
- parent_old: float32 [32, 1024, 1024], P(None, 'tile', 'nest'), may hold values from -6 to 6
- smooth_rate: float32 [32], replicated, may hold values from 0.03 to 0.22
Outputs:
- parent_new: float32 [32, 1024, 1024], P(None, 'tile', 'nest')
The draws below stay inside these ranges and needn't reach their ends.
Inputs may be any that keep to these rules, and one draw needn't show every extreme that they name: nest_offsets[n, 0] lies in 0 .. 512 and nest_offsets[n, 1] in 0 .. 1023. priority[x, y] is -1 or a nest n with nest_offsets[n, 0] <= y < nest_offsets[n, 0] + 512.
All inputs are finite; a program needn't handle non-finite values.
Results may differ from the reference program's by a relative error of at most 0.000058.
Values sent between devices are 32-bit elements; how exact they have to be, the bound alone decides.
A program may use at most 128 MiB of HBM per device.

```python
import math
import jax
import jax.numpy as jnp
from jax import lax

CROW = 24
FL = 32
PRD = 8
PCOLS = 1024
CW = 3072
CROWS_ALL = 1536
NR = 512
PROWS_ALL = 1024
NESTS = 4


def nest_layout(key):
    key_top, key_left, key_score, key_skip, key_order = jax.random.split(jax.random.fold_in(key, 7), 5)
    top_rows = jax.random.randint(key_top, (NESTS,), 0, PROWS_ALL - NR + 1)
    left_cols = jax.random.randint(key_left, (NESTS,), 0, PCOLS)
    order = jax.random.permutation(key_order, NESTS)
    top_rows = top_rows.at[order[0]].set(PROWS_ALL - NR)
    top_rows = top_rows.at[order[1 % NESTS]].set(0)
    left_cols = left_cols.at[order[2 % NESTS]].set(PCOLS - 1)
    left_cols = left_cols.at[order[3 % NESTS]].set(0)
    row_ids = jnp.arange(PROWS_ALL)
    covered = (row_ids[None, :] >= top_rows[:, None]) & (row_ids[None, :] < top_rows[:, None] + NR)
    scores = jax.random.randint(key_score, (NESTS, PCOLS, PROWS_ALL), 0, 1000) * NESTS + jnp.arange(NESTS)[:, None, None]
    scores = jnp.where(covered[:, None, :], scores, -1)
    chosen = jnp.argmax(scores, axis=0).astype(jnp.int32)
    any_cover = jnp.any(covered, axis=0)
    skipped = jax.random.randint(key_skip, (PCOLS, PROWS_ALL), 0, 4) == 0
    priority_map = jnp.where(any_cover[None, :] & jnp.logical_not(skipped), chosen, -1)
    offsets = jnp.stack([top_rows, left_cols], axis=1)
    return (offsets.astype(jnp.int32), priority_map.astype(jnp.int32))


def draw_nest_offsets(key, part):
    return nest_layout(key)[0]


def draw_priority(key, part):
    return nest_layout(key)[1]


def draw_row_weights(key, part):
    tap_weights = jax.random.uniform(key, (PRD, 3), jnp.float32, 0.5, 1.5)
    tap_weights = tap_weights / jnp.sum(tap_weights, axis=1, keepdims=True)
    col_ids = jnp.arange(CROW)
    parent_ids = jnp.arange(PRD)
    matrix = jnp.zeros((PRD, CROW), jnp.float32)
    for member in range(3):
        matrix = matrix + tap_weights[:, member:member + 1] * (col_ids[None, :] == 3 * parent_ids[:, None] + member).astype(jnp.float32)
    return matrix


def draw_col_weights(key, part):
    key_inner, key_outer = jax.random.split(key)
    inner = jax.random.uniform(key_inner, (PCOLS, 3), jnp.float32, 0.5, 1.5)
    outer = jax.random.uniform(key_outer, (PCOLS, 2), jnp.float32, 0.1, 0.5)
    tap_weights = jnp.concatenate([outer[:, :1], inner, outer[:, 1:]], axis=1)
    tap_weights = tap_weights / jnp.sum(tap_weights, axis=1, keepdims=True)
    child_ids = jnp.arange(CW)
    parent_ids = jnp.arange(PCOLS)
    matrix = jnp.zeros((CW, PCOLS), jnp.float32)
    for member in range(5):
        target = (3 * parent_ids + member - 1) % CW
        matrix = matrix + tap_weights[None, :, member] * (child_ids[:, None] == target[None, :]).astype(jnp.float32)
    return matrix


def block_levels(key, extent, pieces, smallest, largest):
    loudness, own = 1.0, jax.random.fold_in(key, 6)
    for dim, shards_of in pieces:
        heights = jnp.exp(jax.random.uniform(jax.random.fold_in(own, dim), (shards_of,), jnp.float32, smallest / len(pieces), largest / len(pieces)))
        loudness = loudness * jnp.repeat(heights, extent[dim] // shards_of).reshape([-1 if axis == dim else 1 for axis in range(len(extent))])
    return loudness


def normal_values(key, dims, deviation, limit, cuts=(), kind=jnp.bfloat16):
    gain = block_levels(key, dims, cuts, -0.22, 0.18) if cuts else 1.0
    entries = jax.random.normal(key, dims, jnp.float32) * deviation * gain
    return jnp.minimum(jnp.maximum(entries, -limit), limit).astype(kind)


def setup_inputs(seed: int = 0) -> dict:
    key_list = jax.random.split(jax.random.key(seed), 8)
    child_fields = normal_values(key_list[0], (NESTS, FL, CROWS_ALL, CW), 3.0, 18.0, ((0, 4), (2, 64)), jnp.float32)
    row_weights = draw_row_weights(jax.random.fold_in(key_list[7], 71), 0)
    col_weights = draw_col_weights(jax.random.fold_in(key_list[7], 71), 0)
    nest_offsets = draw_nest_offsets(jax.random.fold_in(key_list[7], 71), 0)
    priority = draw_priority(jax.random.fold_in(key_list[7], 71), 0)
    parent_old = normal_values(key_list[5], (FL, PCOLS, PROWS_ALL), 1.0, 6.0, ((1, 64), (2, 4)), jnp.float32)
    smooth_rate = jnp.clip(jnp.exp(jax.random.uniform(key_list[6], (FL,), jnp.float32, math.log(0.03), math.log(0.22))), 0.03, 0.22)
    return {"child_fields": child_fields, "row_weights": row_weights, "col_weights": col_weights, "nest_offsets": nest_offsets, "priority": priority, "parent_old": parent_old, "smooth_rate": smooth_rate}


def reference(child_fields, row_weights, col_weights, nest_offsets, priority, parent_old, smooth_rate):
    nest_count, planes, crows_all, child_cols = child_fields.shape
    cell_rows, child_rows = row_weights.shape
    row_blocks = crows_all // child_rows
    nrows = row_blocks * cell_rows

    def restrict_one(child_block):
        grouped = child_block.reshape(planes, row_blocks, child_rows, child_cols)
        thinned = jnp.einsum('pr,ftrc->ftpc', row_weights, grouped, precision=lax.Precision.HIGHEST)
        thinned = thinned.reshape(planes, nrows, child_cols)
        return jnp.einsum('fyc,cx->fxy', thinned, col_weights, precision=lax.Precision.HIGHEST)

    restricted = lax.map(restrict_one, child_fields)
    merged = parent_old
    for nest_num in range(nest_count):
        rolled = jnp.roll(restricted[nest_num], nest_offsets[nest_num, 1], axis=1)
        placed = lax.dynamic_update_slice(jnp.zeros_like(parent_old), rolled,
                                          (jnp.int32(0), jnp.int32(0), nest_offsets[nest_num, 0].astype(jnp.int32)))
        merged = jnp.where((priority == nest_num)[None], placed, merged)
    east_side = jnp.roll(merged, -1, axis=1)
    west_side = jnp.roll(merged, 1, axis=1)
    padded = jnp.concatenate([merged[:, :, :1], merged, merged[:, :, -1:]], axis=2)
    north_side = padded[:, :, 2:]
    south_side = padded[:, :, :-2]
    return merged + smooth_rate[:, None, None] * (east_side + west_side + north_side + south_side - 4.0 * merged)
```

```python
import functools

import jax
import jax.numpy as jnp
from jax import lax
from jax.experimental import pallas as pl
from jax.experimental.pallas import tpu as pltpu
from jax.sharding import PartitionSpec as P

MESH = pl.DeviceIdType.MESH
LANES = 128
F32 = jnp.float32
BF16 = jnp.bfloat16


def split(value):
    high = value.astype(BF16)
    return high, (value - high.astype(F32)).astype(BF16)


def dot(a, b):
    return jnp.dot(a, b, preferred_element_type=F32)


def remote(src, dst, send_sem, recv_sem, where):
    return pltpu.make_async_remote_copy(
        src_ref=src,
        dst_ref=dst,
        send_sem=send_sem,
        recv_sem=recv_sem,
        device_id=where,
        device_id_type=MESH,
    )


def order(groups):
    for g in range(groups):
        yield "R", g
        yield "S", g
    for g in range(groups + 3):
        if g < groups:
            yield "F", g
        if 0 <= g - 1 < groups:
            yield "M", g - 1
        if 0 <= g - 2 < groups:
            yield "E", g - 2


def kernel(
    tiles,
    nests,
    offs_ref,
    rate_ref,
    rw_hbm,
    prio_hbm,
    child_hbm,
    cw_hbm,
    parent_hbm,
    result,
    rw_ref,
    prio_ref,
    child,
    cw,
    cw_high,
    cw_low,
    merged,
    pieces,
    strips,
    blocks,
    slabs,
    ew_out,
    ew_in,
    ns_out,
    ns_in,
    small_sem,
    child_sem,
    cw_sem,
    parent_sem,
    a2a_send,
    a2a_recv,
    slab_send,
    slab_recv,
    edge_send,
    edge_recv,
):
    planes, crow, ccols = child.shape
    prd = rw_ref.shape[0]
    cols, rows = prio_ref.shape
    per = LANES // cols
    groups = planes // per
    nrows = prd * tiles
    m = per * prd
    me_n, me_t = lax.axis_index("nest"), lax.axis_index("tile")

    def group(ref, g):
        return ref.at[pl.ds(g * per, per)]

    child_in = [
        pltpu.make_async_copy(group(child_hbm.at[0], g), group(child, g), child_sem.at[g])
        for g in range(groups)
    ]
    chunks = cw_sem.shape[0]
    depth = ccols // chunks
    cw_in = [
        pltpu.make_async_copy(
            cw_hbm.at[pl.ds(k * depth, depth)], cw.at[pl.ds(k * depth, depth)], cw_sem.at[k]
        )
        for k in range(chunks)
    ]
    parent_in = pltpu.make_async_copy(parent_hbm, merged, parent_sem)
    rw_in = pltpu.make_async_copy(rw_hbm, rw_ref, small_sem.at[0])
    prio_in = pltpu.make_async_copy(prio_hbm, prio_ref, small_sem.at[1])
    rw_in.start()
    child_in[0].start()
    for k in range(chunks):
        cw_in[k].start()
    for g in range(1, groups):
        child_in[g].start()
    prio_in.start()
    parent_in.start()
    barrier = pltpu.get_barrier_semaphore()
    for d in range(1, tiles):
        pl.semaphore_signal(
            barrier, inc=1, device_id={"tile": lax.rem(me_t + d, tiles)}, device_id_type=MESH
        )
    for d in range(1, nests):
        pl.semaphore_signal(
            barrier, inc=1, device_id={"nest": lax.rem(me_n + d, nests)}, device_id_type=MESH
        )

    rw_in.wait()
    rw = rw_ref[...]
    spread_rows = lax.broadcasted_iota(jnp.int32, (per * crow, crow), 0)
    spread_cols = lax.broadcasted_iota(jnp.int32, (per * crow, crow), 1)
    spread = jnp.where(lax.rem(spread_rows, crow) == spread_cols, 1.0, 0.0).astype(BF16)
    wide_r = lax.broadcasted_iota(jnp.int32, (m, per * crow), 0)
    wide_c = lax.broadcasted_iota(jnp.int32, (m, per * crow), 1)
    diagonal = wide_r // prd == wide_c // crow
    block_rw = []
    for part in split(rw):
        line = lax.dot_general(
            part, spread, (((1,), (1,)), ((), ())), preferred_element_type=F32
        )
        line = jnp.concatenate([line] * per, axis=0)
        block_rw.append(jnp.where(diagonal, line, 0.0).astype(BF16))
    both_rw = jnp.concatenate(block_rw, axis=0)

    lane_group = lax.broadcasted_iota(jnp.int32, (prd, LANES), 1) // cols
    left, top = jnp.int32(0), jnp.int32(0)
    for n in range(nests):
        left = jnp.where(me_n == n, offs_ref[1, n], left)
        top = jnp.where(me_n == n, offs_ref[0, n], top)
    top = lax.rem(top, nrows)

    here = pl.ds(pl.multiple_of(me_t * prd, prd), prd)

    def fold(both, high, b_high, b_low):
        wide = dot(both, b_high)
        return (wide[:m] + wide[m:]) + dot(high, b_low)

    def restrict(g):
        child_in[g].wait()
        block = child[g * per : (g + 1) * per].reshape(per * crow, ccols)
        thinned = fold(both_rw, block_rw[0], *split(block))
        high, low = split(thinned)
        both = jnp.concatenate([high, low], axis=0)
        if g == 0:
            restricted = None
            for k in range(chunks):
                part = slice(k * depth, (k + 1) * depth)
                cw_in[k].wait()
                w_high, w_low = split(cw[part])
                cw_high[part] = w_high
                cw_low[part] = w_low
                now = fold(both[:, part], high[:, part], w_high, w_low)
                restricted = now if k == 0 else restricted + now
        else:
            restricted = fold(both, high, cw_high[...], cw_low[...])
        restricted = pltpu.roll(restricted, left, 1)
        for t in range(tiles):
            base, off = (t * cols) // LANES * LANES, (t * cols) % LANES
            piece = None
            for j in range(per):
                part = restricted[j * prd : (j + 1) * prd, base : base + LANES]
                shift = (j * cols - off) % LANES
                if shift:
                    part = pltpu.roll(part, shift, 1)
                piece = part if j == 0 else jnp.where(lane_group == j, part, piece)
            pieces[g, t] = piece
        strips[g, here, :] = pieces[g, me_t]

    def send(g):
        if g == 0:
            pl.semaphore_wait(barrier, tiles + nests - 2)
        for d in range(1, tiles):
            t = lax.rem(me_t + d, tiles)
            remote(
                pieces.at[g, t],
                strips.at[g, here, :],
                a2a_send.at[g],
                a2a_recv.at[g],
                {"tile": t},
            ).start()

    def a2a_bytes(g):
        most = strips.at[g, pl.ds(0, prd * (tiles - 1)), :]
        return remote(most, most, a2a_send.at[g], a2a_recv.at[g], {"tile": me_t})

    slab_out = []

    def forward(g):
        a2a_bytes(g).wait_recv()
        turned = pltpu.roll(strips[g].T, top, 1)
        for b in range(nrows // rows):
            blocks[g, b] = turned[:, b * rows : (b + 1) * rows]
        for d in range(1, nests):
            to = lax.rem(me_n + d, nests)
            copy = remote(
                blocks.at[g, lax.rem(to, nrows // rows)],
                slabs.at[g, d - 1],
                slab_send.at[g, d - 1],
                slab_recv.at[g, d - 1],
                {"nest": to},
            )
            copy.start()
            slab_out.append(copy)

    prio_in.wait()
    prio = prio_ref[...]
    west_t, east_t = lax.rem(me_t + tiles - 1, tiles), lax.rem(me_t + 1, tiles)
    low_n, high_n = lax.rem(me_n + nests - 1, nests), lax.rem(me_n + 1, nests)
    lane = lax.broadcasted_iota(jnp.int32, (cols, LANES), 1)

    edges = {}

    def merge(g):
        if g == 0:
            parent_in.wait()
        now = merged[g * per : (g + 1) * per]
        mine = blocks[g, lax.rem(me_n, nrows // rows)].reshape(per, cols, rows)
        now = jnp.where((prio == me_n)[None], mine, now)
        for d in range(1, nests):
            slab_out[g * (nests - 1) + d - 1].wait_recv()
            there = lax.rem(me_n + nests - d, nests)
            now = jnp.where((prio == there)[None], slabs[g, d - 1].reshape(per, cols, rows), now)
        merged[g * per : (g + 1) * per] = now
        low = jnp.zeros((cols, LANES), F32)
        high = jnp.zeros((cols, LANES), F32)
        for j in range(per):
            low = jnp.where(lane == j, now[j, :, :1], low)
            high = jnp.where(lane == j, now[j, :, rows - 1 :], high)
            ew_out[g, 0, j : j + 1] = now[j, :1]
            ew_out[g, 1, j : j + 1] = now[j, cols - 1 :]
        ns_out[g, 0] = low
        ns_out[g, 1] = high
        for side, (source, target, where) in enumerate(
            (
                (ew_out.at[g, 0], ew_in.at[g, 0], {"tile": west_t}),
                (ew_out.at[g, 1], ew_in.at[g, 1], {"tile": east_t}),
                (ns_out.at[g, 0], ns_in.at[g, 0], {"nest": low_n}),
                (ns_out.at[g, 1], ns_in.at[g, 1], {"nest": high_n}),
            )
        ):
            copy = remote(source, target, edge_send.at[g, side], edge_recv.at[g, side], where)
            copy.start()
            edges[g, side] = copy

    row_lane = lax.broadcasted_iota(jnp.int32, (cols, rows), 1)

    def finish(g):
        for side in range(4):
            edges[g, side].wait_recv()
        for j in range(per):
            f = g * per + j
            now = merged[f]
            east = jnp.concatenate([now[1:], ew_in[g, 0, j : j + 1]], axis=0)
            west = jnp.concatenate([ew_in[g, 1, j : j + 1], now[:-1]], axis=0)
            above = jnp.where(me_n == nests - 1, now[:, rows - 1 :], ns_in[g, 0, :, j : j + 1])
            below = jnp.where(me_n == 0, now[:, :1], ns_in[g, 1, :, j : j + 1])
            north = jnp.where(row_lane == rows - 1, above, pltpu.roll(now, rows - 1, 1))
            south = jnp.where(row_lane == 0, below, pltpu.roll(now, 1, 1))
            result[f] = now + rate_ref[f] * (east + west + north + south - 4.0 * now)

    stages = {"R": restrict, "S": send, "F": forward, "M": merge, "E": finish}
    for step in order(groups):
        stages[step[0]](step[1])

    for g in range(groups):
        a2a_bytes(g).wait_send()
    for copy in slab_out + list(edges.values()):
        copy.wait_send()


def per_device(
    child_fields, row_weights, col_weights, nest_offsets, priority, parent_old, smooth_rate
):
    planes, crow, ccols = child_fields.shape[1:]
    prd = row_weights.shape[0]
    _, cols, rows = parent_old.shape
    tiles, nests = lax.axis_size("tile"), lax.axis_size("nest")
    per = LANES // cols
    groups = planes // per
    nrows = prd * tiles
    smem = pl.BlockSpec(memory_space=pltpu.SMEM)
    hbm = pl.BlockSpec(memory_space=pl.ANY)
    dma = pltpu.SemaphoreType.DMA
    return pl.pallas_call(
        functools.partial(kernel, tiles, nests),
        out_shape=pltpu.VMEM(parent_old.shape, F32),
        in_specs=[smem, smem] + [hbm] * 5,
        out_specs=pl.BlockSpec(memory_space=pltpu.VMEM),
        scratch_shapes=[
            pltpu.VMEM(row_weights.shape, F32),
            pltpu.VMEM((cols, rows), jnp.int32),
            pltpu.VMEM((planes, crow, ccols), F32),
            pltpu.VMEM(col_weights.shape, F32),
            pltpu.VMEM(col_weights.shape, BF16),
            pltpu.VMEM(col_weights.shape, BF16),
            pltpu.VMEM((planes, cols, rows), F32),
            pltpu.VMEM((groups, tiles, prd, LANES), F32),
            pltpu.VMEM((groups, nrows, LANES), F32),
            pltpu.VMEM((groups, nrows // rows, LANES, rows), F32),
            pltpu.VMEM((groups, nests - 1, LANES, rows), F32),
            pltpu.VMEM((groups, 2, per, rows), F32),
            pltpu.VMEM((groups, 2, per, rows), F32),
            pltpu.VMEM((groups, 2, cols, LANES), F32),
            pltpu.VMEM((groups, 2, cols, LANES), F32),
            dma((2,)),
            dma((groups,)),
            dma((6,)),
            dma,
            dma((groups,)),
            dma((groups,)),
            dma((groups, nests - 1)),
            dma((groups, nests - 1)),
            dma((groups, 4)),
            dma((groups, 4)),
        ],
        compiler_params=pltpu.CompilerParams(
            collective_id=0, has_side_effects=True, vmem_limit_bytes=60 * 2**20
        ),
    )(nest_offsets.T, smooth_rate, row_weights, priority, child_fields, col_weights, parent_old)


def solution(mesh):
    return jax.shard_map(
        per_device,
        mesh=mesh,
        in_specs=(
            P("nest", None, "tile", None),
            P(),
            P(),
            P(),
            P("tile", "nest"),
            P(None, "tile", "nest"),
            P(),
        ),
        out_specs=P(None, "tile", "nest"),
        check_vma=False,
    )
```

```python
import functools

import jax
import jax.numpy as jnp
from jax import lax
from jax.experimental import pallas as pl
from jax.experimental.pallas import tpu as pltpu
from jax.sharding import PartitionSpec as P

MESH = pl.DeviceIdType.MESH
LANES = 128
F32 = jnp.float32
BF16 = jnp.bfloat16
CHUNKS = 6
AHEAD = 3


def split(value):
    high = value.astype(BF16)
    return high, (value - high.astype(F32)).astype(BF16)


def dot(a, b):
    return jnp.dot(a, b, preferred_element_type=F32)


def remote(src, dst, send_sem, recv_sem, where):
    return pltpu.make_async_remote_copy(
        src_ref=src,
        dst_ref=dst,
        send_sem=send_sem,
        recv_sem=recv_sem,
        device_id=where,
        device_id_type=MESH,
    )


def order(groups):
    for g in range(groups + 3):
        if g < groups:
            yield "F", g
        if 0 <= g - 1 < groups:
            yield "M", g - 1
        if 0 <= g - 2 < groups:
            yield "E", g - 2


def kernel(
    tiles,
    nests,
    offs_hbm,
    rate_hbm,
    rw_hbm,
    prio_hbm,
    child_hbm,
    cw_hbm,
    parent_hbm,
    result,
    offs_ref,
    rate_ref,
    rw_ref,
    prio_ref,
    child,
    cw,
    cw_high,
    cw_low,
    both_ref,
    restricted_ref,
    merged,
    pieces,
    strips,
    blocks,
    slabs,
    ew_out,
    ew_in,
    ns_out,
    ns_in,
    small_sem,
    child_sem,
    cw_sem,
    parent_sem,
    a2a_send,
    a2a_recv,
    slab_send,
    slab_recv,
    edge_send,
    edge_recv,
):
    planes, crow, ccols = child.shape
    prd = rw_ref.shape[0]
    cols, rows = prio_ref.shape
    per = LANES // cols
    groups = planes // per
    nrows = prd * tiles
    m = per * prd
    me_n, me_t = lax.axis_index("nest"), lax.axis_index("tile")

    def child_in(g):
        fields = pl.ds(g * per, per)
        return pltpu.make_async_copy(child_hbm.at[0, fields], child.at[fields], child_sem.at[g])

    chunks = cw_sem.shape[0]
    depth = ccols // chunks

    def cw_in(k):
        part = pl.ds(pl.multiple_of(k * depth, depth), depth)
        return pltpu.make_async_copy(cw_hbm.at[part], cw.at[part], cw_sem.at[k])

    parent_in = pltpu.make_async_copy(parent_hbm, merged, parent_sem)
    rw_in = pltpu.make_async_copy(rw_hbm, rw_ref, small_sem.at[0])
    prio_in = pltpu.make_async_copy(prio_hbm, prio_ref, small_sem.at[1])
    offs_in = pltpu.make_async_copy(offs_hbm, offs_ref, small_sem.at[2])
    rate_in = pltpu.make_async_copy(rate_hbm, rate_ref, small_sem.at[3])
    rw_in.start()
    child_in(0).start()
    for k in range(AHEAD):
        cw_in(k).start()
    offs_in.start()
    rate_in.start()
    prio_in.start()
    barrier = pltpu.get_barrier_semaphore()

    def greet_tile(d, carry):
        pl.semaphore_signal(
            barrier, inc=1, device_id={"tile": lax.rem(me_t + d, tiles)}, device_id_type=MESH
        )
        return carry

    lax.fori_loop(1, tiles, greet_tile, 0)
    for d in range(1, nests):
        pl.semaphore_signal(
            barrier, inc=1, device_id={"nest": lax.rem(me_n + d, nests)}, device_id_type=MESH
        )

    rw_in.wait()
    rw = rw_ref[...]
    spread_rows = lax.broadcasted_iota(jnp.int32, (per * crow, crow), 0)
    spread_cols = lax.broadcasted_iota(jnp.int32, (per * crow, crow), 1)
    spread = jnp.where(lax.rem(spread_rows, crow) == spread_cols, 1.0, 0.0).astype(BF16)
    wide_r = lax.broadcasted_iota(jnp.int32, (m, per * crow), 0)
    wide_c = lax.broadcasted_iota(jnp.int32, (m, per * crow), 1)
    diagonal = wide_r // prd == wide_c // crow
    block_rw = []
    for part in split(rw):
        line = lax.dot_general(
            part, spread, (((1,), (1,)), ((), ())), preferred_element_type=F32
        )
        line = jnp.concatenate([line] * per, axis=0)
        block_rw.append(jnp.where(diagonal, line, 0.0).astype(BF16))
    both_rw = jnp.concatenate(block_rw, axis=0)

    lane_group = lax.broadcasted_iota(jnp.int32, (prd, LANES), 1) // cols
    offs_in.wait()
    rate_in.wait()
    left, top = jnp.int32(0), jnp.int32(0)
    for n in range(nests):
        left = jnp.where(me_n == n, offs_ref[1, n], left)
        top = jnp.where(me_n == n, offs_ref[0, n], top)
    top = lax.rem(top, nrows)

    here = pl.ds(pl.multiple_of(me_t * prd, prd), prd)

    def fold(both, high, b_high, b_low):
        wide = dot(both, b_high)
        return (wide[:m] + wide[m:]) + dot(high, b_low)

    def thin(g):
        child_in(g).wait()
        block = child[pl.ds(g * per, per)].reshape(per * crow, ccols)
        thinned = fold(both_rw, block_rw[0], *split(block))
        high, low = split(thinned)
        both_ref[:m] = high
        both_ref[m:] = low

    def cut(g):
        restricted = pltpu.roll(restricted_ref[...], left, 1)
        for base in range(0, tiles * cols, LANES):
            parts = [restricted[j * prd : (j + 1) * prd, base : base + LANES] for j in range(per)]
            step = per // 2
            while step:
                for a in range(per):
                    if a & step:
                        continue
                    one, two = parts[a], parts[a + step]
                    keep = lane_group & step == 0
                    parts[a] = jnp.where(keep, one, pltpu.roll(two, step * cols, 1))
                    parts[a + step] = jnp.where(keep, pltpu.roll(one, LANES - step * cols, 1), two)
                step //= 2
            for q in range(per):
                pieces[g, base // cols + q] = parts[q]
        strips[g, here, :] = pieces[g, me_t]

    def send(g):
        def send_one(d, carry):
            t = lax.rem(me_t + d, tiles)
            remote(
                pieces.at[g, t],
                strips.at[g, here, :],
                a2a_send.at[g],
                a2a_recv.at[g],
                {"tile": t},
            ).start()
            return carry

        lax.fori_loop(1, tiles, send_one, 0)

    def first():
        thin(0)
        for k in range(chunks):
            part = slice(k * depth, (k + 1) * depth)
            cw_in(k).wait()
            if k + AHEAD < chunks:
                cw_in(k + AHEAD).start()
            for g in range(1, groups):
                if k == min(chunks - AHEAD + g - 1, chunks - 1):
                    child_in(g).start()
            w_high, w_low = split(cw[part])
            cw_high[part] = w_high
            cw_low[part] = w_low
            now = fold(both_ref[:, part], both_ref[:m, part], w_high, w_low)
            restricted_ref[...] = now if k == 0 else restricted_ref[...] + now
        cut(0)
        parent_in.start()
        pl.semaphore_wait(barrier, tiles + nests - 2)
        send(0)

    def restrict(g, carry):
        thin(g)
        restricted_ref[...] = fold(both_ref[...], both_ref[:m], cw_high[...], cw_low[...])
        cut(g)
        send(g)
        return carry

    def a2a_bytes(g):
        most = strips.at[g, pl.ds(0, prd * (tiles - 1)), :]
        return remote(most, most, a2a_send.at[g], a2a_recv.at[g], {"tile": me_t})

    slab_out = []

    def forward(g):
        a2a_bytes(g).wait_recv()
        turned = pltpu.roll(strips[g].T, top, 1)
        for b in range(nrows // rows):
            blocks[g, b] = turned[:, b * rows : (b + 1) * rows]
        for d in range(1, nests):
            to = lax.rem(me_n + d, nests)
            copy = remote(
                blocks.at[g, lax.rem(to, nrows // rows)],
                slabs.at[g, d - 1],
                slab_send.at[g, d - 1],
                slab_recv.at[g, d - 1],
                {"nest": to},
            )
            copy.start()
            slab_out.append(copy)

    prio_in.wait()
    prio = prio_ref[...]
    west_t, east_t = lax.rem(me_t + tiles - 1, tiles), lax.rem(me_t + 1, tiles)
    low_n, high_n = lax.rem(me_n + nests - 1, nests), lax.rem(me_n + 1, nests)
    lane = lax.broadcasted_iota(jnp.int32, (cols, LANES), 1)

    edges = {}

    def merge(g):
        if g == 0:
            parent_in.wait()
        now = merged[g * per : (g + 1) * per]
        mine = blocks[g, lax.rem(me_n, nrows // rows)].reshape(per, cols, rows)
        now = jnp.where((prio == me_n)[None], mine, now)
        for d in range(1, nests):
            slab_out[g * (nests - 1) + d - 1].wait_recv()
            there = lax.rem(me_n + nests - d, nests)
            now = jnp.where((prio == there)[None], slabs[g, d - 1].reshape(per, cols, rows), now)
        merged[g * per : (g + 1) * per] = now
        low = jnp.zeros((cols, LANES), F32)
        high = jnp.zeros((cols, LANES), F32)
        for j in range(per):
            low = jnp.where(lane == j, now[j, :, :1], low)
            high = jnp.where(lane == j, now[j, :, rows - 1 :], high)
            ew_out[g, 0, j : j + 1] = now[j, :1]
            ew_out[g, 1, j : j + 1] = now[j, cols - 1 :]
        ns_out[g, 0] = low
        ns_out[g, 1] = high
        for side, (source, target, where) in enumerate(
            (
                (ew_out.at[g, 0], ew_in.at[g, 0], {"tile": west_t}),
                (ew_out.at[g, 1], ew_in.at[g, 1], {"tile": east_t}),
                (ns_out.at[g, 0], ns_in.at[g, 0], {"nest": low_n}),
                (ns_out.at[g, 1], ns_in.at[g, 1], {"nest": high_n}),
            )
        ):
            copy = remote(source, target, edge_send.at[g, side], edge_recv.at[g, side], where)
            copy.start()
            edges[g, side] = copy

    row_lane = lax.broadcasted_iota(jnp.int32, (cols, rows), 1)

    def finish(g):
        for side in range(4):
            edges[g, side].wait_recv()
        for j in range(per):
            f = g * per + j
            now = merged[f]
            east = jnp.concatenate([now[1:], ew_in[g, 0, j : j + 1]], axis=0)
            west = jnp.concatenate([ew_in[g, 1, j : j + 1], now[:-1]], axis=0)
            above = jnp.where(me_n == nests - 1, now[:, rows - 1 :], ns_in[g, 0, :, j : j + 1])
            below = jnp.where(me_n == 0, now[:, :1], ns_in[g, 1, :, j : j + 1])
            north = jnp.where(row_lane == rows - 1, above, pltpu.roll(now, rows - 1, 1))
            south = jnp.where(row_lane == 0, below, pltpu.roll(now, 1, 1))
            result[f] = now + rate_ref[f] * (east + west + north + south - 4.0 * now)

    first()
    lax.fori_loop(1, groups, restrict, 0)
    stages = {"F": forward, "M": merge, "E": finish}
    for step in order(groups):
        stages[step[0]](step[1])

    for g in range(groups):
        a2a_bytes(g).wait_send()
    for copy in slab_out + list(edges.values()):
        copy.wait_send()


def per_device(
    child_fields, row_weights, col_weights, nest_offsets, priority, parent_old, smooth_rate
):
    planes, crow, ccols = child_fields.shape[1:]
    prd = row_weights.shape[0]
    _, cols, rows = parent_old.shape
    tiles, nests = lax.axis_size("tile"), lax.axis_size("nest")
    per = LANES // cols
    groups = planes // per
    nrows = prd * tiles
    hbm = pl.BlockSpec(memory_space=pl.ANY)
    dma = pltpu.SemaphoreType.DMA
    return pl.pallas_call(
        functools.partial(kernel, tiles, nests),
        out_shape=pltpu.VMEM(parent_old.shape, F32),
        in_specs=[hbm] * 7,
        out_specs=pl.BlockSpec(memory_space=pltpu.VMEM),
        scratch_shapes=[
            pltpu.SMEM((2, nests), jnp.int32),
            pltpu.SMEM((planes,), F32),
            pltpu.VMEM(row_weights.shape, F32),
            pltpu.VMEM((cols, rows), jnp.int32),
            pltpu.VMEM((planes, crow, ccols), F32),
            pltpu.VMEM(col_weights.shape, F32),
            pltpu.VMEM(col_weights.shape, BF16),
            pltpu.VMEM(col_weights.shape, BF16),
            pltpu.VMEM((2 * per * prd, ccols), BF16),
            pltpu.VMEM((per * prd, col_weights.shape[1]), F32),
            pltpu.VMEM((planes, cols, rows), F32),
            pltpu.VMEM((groups, tiles, prd, LANES), F32),
            pltpu.VMEM((groups, nrows, LANES), F32),
            pltpu.VMEM((groups, nrows // rows, LANES, rows), F32),
            pltpu.VMEM((groups, nests - 1, LANES, rows), F32),
            pltpu.VMEM((groups, 2, per, rows), F32),
            pltpu.VMEM((groups, 2, per, rows), F32),
            pltpu.VMEM((groups, 2, cols, LANES), F32),
            pltpu.VMEM((groups, 2, cols, LANES), F32),
            dma((4,)),
            dma((groups,)),
            dma((CHUNKS,)),
            dma,
            dma((groups,)),
            dma((groups,)),
            dma((groups, nests - 1)),
            dma((groups, nests - 1)),
            dma((groups, 4)),
            dma((groups, 4)),
        ],
        compiler_params=pltpu.CompilerParams(
            collective_id=0, has_side_effects=True, vmem_limit_bytes=60 * 2**20
        ),
    )(nest_offsets.T, smooth_rate, row_weights, priority, child_fields, col_weights, parent_old)


def solution(mesh):
    return jax.shard_map(
        per_device,
        mesh=mesh,
        in_specs=(
            P("nest", None, "tile", None),
            P(),
            P(),
            P(),
            P("tile", "nest"),
            P(None, "tile", "nest"),
            P(),
        ),
        out_specs=P(None, "tile", "nest"),
        check_vma=False,
    )
```

```python
import functools

import jax
import jax.numpy as jnp
from jax import lax
from jax.experimental import pallas as pl
from jax.experimental.pallas import tpu as pltpu
from jax.sharding import PartitionSpec as P

MESH = pl.DeviceIdType.MESH
LANES = 128
F32 = jnp.float32
BF16 = jnp.bfloat16
CHUNKS = 6
AHEAD = 3
SPAN = 2


def split(value):
    high = value.astype(BF16)
    return high, (value - high.astype(F32)).astype(BF16)


def dot(a, b):
    return jnp.dot(a, b, preferred_element_type=F32)


def remote(src, dst, send_sem, recv_sem, where):
    return pltpu.make_async_remote_copy(
        src_ref=src,
        dst_ref=dst,
        send_sem=send_sem,
        recv_sem=recv_sem,
        device_id=where,
        device_id_type=MESH,
    )


def order(groups):
    for g in range(groups + 2):
        if g < groups:
            yield "F", g
        if 0 <= g - 1 < groups:
            yield "M", g - 1
        if 0 <= g - 2 < groups:
            yield "E", g - 2
        if g < groups:
            yield "P", g


def kernel(
    tiles,
    nests,
    offs_hbm,
    rate_hbm,
    rw_hbm,
    prio_hbm,
    child_hbm,
    cw_hbm,
    parent_hbm,
    result,
    offs_ref,
    rate_ref,
    rw_ref,
    prio_ref,
    child,
    cw,
    cw_high,
    cw_low,
    both_ref,
    restricted_ref,
    merged,
    pieces,
    strips,
    blocks,
    via,
    relayed,
    slabs,
    prio_near,
    ew_out,
    ew_in,
    ns_out,
    ns_in,
    small_sem,
    child_sem,
    cw_sem,
    parent_sem,
    a2a_send,
    a2a_recv,
    near_send,
    near_recv,
    via_send,
    via_recv,
    slab_send,
    slab_recv,
    edge_send,
    edge_recv,
):
    planes, crow, ccols = child.shape
    prd = rw_ref.shape[0]
    cols, rows = prio_ref.shape
    per = LANES // cols
    groups = planes // per
    nrows = prd * tiles
    m = per * prd
    me_n, me_t = lax.axis_index("nest"), lax.axis_index("tile")

    def child_in(g):
        fields = pl.ds(g * per, per)
        return pltpu.make_async_copy(child_hbm.at[0, fields], child.at[fields], child_sem.at[g])

    chunks = cw_sem.shape[0]
    depth = ccols // chunks

    def cw_in(k):
        part = pl.ds(pl.multiple_of(k * depth, depth), depth)
        return pltpu.make_async_copy(cw_hbm.at[part], cw.at[part], cw_sem.at[k])

    parent_in = pltpu.make_async_copy(parent_hbm, merged, parent_sem)
    rw_in = pltpu.make_async_copy(rw_hbm, rw_ref, small_sem.at[0])
    prio_in = pltpu.make_async_copy(prio_hbm, prio_ref, small_sem.at[1])
    offs_in = pltpu.make_async_copy(offs_hbm, offs_ref, small_sem.at[2])
    rate_in = pltpu.make_async_copy(rate_hbm, rate_ref, small_sem.at[3])
    rw_in.start()
    child_in(0).start()
    for k in range(AHEAD):
        cw_in(k).start()
    offs_in.start()
    rate_in.start()
    prio_in.start()
    barrier = pltpu.get_barrier_semaphore()

    def greet_tile(d, carry):
        pl.semaphore_signal(
            barrier, inc=1, device_id={"tile": lax.rem(me_t + d, tiles)}, device_id_type=MESH
        )
        return carry

    lax.fori_loop(1, tiles, greet_tile, 0)
    for d in range(1, nests):
        pl.semaphore_signal(
            barrier, inc=1, device_id={"nest": lax.rem(me_n + d, nests)}, device_id_type=MESH
        )

    rw_in.wait()
    rw = rw_ref[...]
    spread_rows = lax.broadcasted_iota(jnp.int32, (per * crow, crow), 0)
    spread_cols = lax.broadcasted_iota(jnp.int32, (per * crow, crow), 1)
    spread = jnp.where(lax.rem(spread_rows, crow) == spread_cols, 1.0, 0.0).astype(BF16)
    wide_r = lax.broadcasted_iota(jnp.int32, (m, per * crow), 0)
    wide_c = lax.broadcasted_iota(jnp.int32, (m, per * crow), 1)
    diagonal = wide_r // prd == wide_c // crow
    block_rw = []
    for part in split(rw):
        line = lax.dot_general(
            part, spread, (((1,), (1,)), ((), ())), preferred_element_type=F32
        )
        line = jnp.concatenate([line] * per, axis=0)
        block_rw.append(jnp.where(diagonal, line, 0.0).astype(BF16))
    both_rw = jnp.concatenate(block_rw, axis=0)

    lane_group = lax.broadcasted_iota(jnp.int32, (prd, LANES), 1) // cols
    offs_in.wait()
    rate_in.wait()
    left, top = jnp.int32(0), jnp.int32(0)
    for n in range(nests):
        left = jnp.where(me_n == n, offs_ref[1, n], left)
        top = jnp.where(me_n == n, offs_ref[0, n], top)
    top = lax.rem(top, nrows)

    here = pl.ds(pl.multiple_of(me_t * prd, prd), prd)

    def fold(both, high, b_high, b_low):
        wide = dot(both, b_high)
        return (wide[:m] + wide[m:]) + dot(high, b_low)

    def thin(g):
        block = child[pl.ds(g * per, per)].reshape(per * crow, ccols)
        thinned = fold(both_rw, block_rw[0], *split(block))
        high, low = split(thinned)
        both_ref[:m] = high
        both_ref[m:] = low

    def cut(g):
        restricted = pltpu.roll(restricted_ref[...], left, 1)
        for base in range(0, tiles * cols, LANES):
            parts = [restricted[j * prd : (j + 1) * prd, base : base + LANES] for j in range(per)]
            step = per // 2
            while step:
                for a in range(per):
                    if a & step:
                        continue
                    one, two = parts[a], parts[a + step]
                    keep = lane_group & step == 0
                    parts[a] = jnp.where(keep, one, pltpu.roll(two, step * cols, 1))
                    parts[a + step] = jnp.where(keep, pltpu.roll(one, LANES - step * cols, 1), two)
                step //= 2
            for q in range(per):
                pieces[g, base // cols + q] = parts[q]
        strips[g, here, :] = pieces[g, me_t]

    def send(g):
        def send_one(d, carry):
            t = lax.rem(me_t + d, tiles)
            remote(
                pieces.at[g, t],
                strips.at[g, here, :],
                a2a_send.at[g],
                a2a_recv.at[g],
                {"tile": t},
            ).start()
            return carry

        lax.fori_loop(1, tiles, send_one, 0)

    def first():
        child_in(0).wait()
        cw_in(AHEAD).start()
        thin(0)
        for k in range(0, chunks, SPAN):
            part = slice(k * depth, (k + SPAN) * depth)
            for c in range(k, k + SPAN):
                cw_in(c).wait()
                if c + AHEAD + 1 < chunks:
                    cw_in(c + AHEAD + 1).start()
                for g in range(1, groups):
                    if c == min(chunks - AHEAD - 2 + g, chunks - 1):
                        child_in(g).start()
            w_high, w_low = split(cw[part])
            cw_high[part] = w_high
            cw_low[part] = w_low
            now = fold(both_ref[:, part], both_ref[:m, part], w_high, w_low)
            restricted_ref[...] = now if k == 0 else restricted_ref[...] + now
        cut(0)
        parent_in.start()
        pl.semaphore_wait(barrier, tiles + nests - 2)
        swap_priorities()
        send(0)

    def restrict(g, carry):
        child_in(g).wait()
        thin(g)
        restricted_ref[...] = fold(both_ref[...], both_ref[:m], cw_high[...], cw_low[...])
        cut(g)
        send(g)
        return carry

    def a2a_bytes(g):
        most = strips.at[g, pl.ds(0, prd * (tiles - 1)), :]
        return remote(most, most, a2a_send.at[g], a2a_recv.at[g], {"tile": me_t})

    prio_in.wait()
    prio = prio_ref[...]
    west_t, east_t = lax.rem(me_t + tiles - 1, tiles), lax.rem(me_t + 1, tiles)
    low_n, high_n = lax.rem(me_n + nests - 1, nests), lax.rem(me_n + 1, nests)
    lane = lax.broadcasted_iota(jnp.int32, (cols, LANES), 1)

    near = lax.rem(me_n + 1, 2)
    half = LANES // 2
    halves = pl.ds(0, half), pl.ds(half, half)
    sent = {}

    def pass_on(key, source, target, sems, to):
        copy = remote(source, target, *sems, {"nest": to})
        copy.start()
        sent[key] = copy

    def swap_priorities():
        for side, to in enumerate((high_n, low_n)):
            sems = near_send.at[side], near_recv.at[side]
            pass_on(("prio", side), prio_ref, prio_near.at[side], sems, to)

    def forward(g):
        a2a_bytes(g).wait_recv()
        turned = pltpu.roll(strips[g].T, top, 1)
        for b in range(nrows // rows):
            blocks[g, b] = turned[:, b * rows : (b + 1) * rows]
        for side, to in enumerate((high_n, low_n)):
            source = blocks.at[g, 1 - near, halves[side]]
            sems = via_send.at[g, side], via_recv.at[g, side]
            pass_on(("via", g, side), source, via.at[g, side], sems, to)
        for side, to in enumerate((high_n, low_n)):
            part = halves[1 - side]
            sems = slab_send.at[g, side], slab_recv.at[g, side]
            source = blocks.at[g, near, part]
            pass_on(("slab", g, side), source, slabs.at[g, side, part], sems, to)

    def relay(g):
        if g == 0:
            for side in range(2):
                sent["prio", side].wait_recv()
        for side, to in enumerate((high_n, low_n)):
            sent["via", g, side].wait_recv()
            origin = (low_n, high_n)[side]
            theirs = (prio_near[1 - side] == origin)[None]
            far = via[g, side].reshape(per // 2, cols, rows)
            own = blocks[g, near, side * half : (side + 1) * half].reshape(per // 2, cols, rows)
            relayed[g, side] = jnp.where(theirs, far, own).reshape(half, rows)
            sems = slab_send.at[g, 2 + side], slab_recv.at[g, 2 + side]
            target = slabs.at[g, side, halves[side]]
            pass_on(("slab", g, 2 + side), relayed.at[g, side], target, sems, to)

    edges = {}

    def merge(g):
        if g == 0:
            parent_in.wait()
        now = merged[g * per : (g + 1) * per]
        mine = blocks[g, lax.rem(me_n, nrows // rows)].reshape(per, cols, rows)
        now = jnp.where((prio == me_n)[None], mine, now)
        for q in range(4):
            sent["slab", g, q].wait_recv()
        far_n = lax.rem(me_n + 2, nests)
        ways = [(prio == n)[None] for n in (low_n, high_n)]
        far = (prio == far_n)[None]
        mixed = []
        for side in range(2):
            part = now[side * (per // 2) : (side + 1) * (per // 2)]
            for way in range(2):
                take = (ways[way] | far) if way == side else ways[way]
                slab = slabs[g, way, side * half : (side + 1) * half]
                part = jnp.where(take, slab.reshape(per // 2, cols, rows), part)
            mixed.append(part)
        now = jnp.concatenate(mixed, axis=0)
        merged[g * per : (g + 1) * per] = now
        low = jnp.zeros((cols, LANES), F32)
        high = jnp.zeros((cols, LANES), F32)
        for j in range(per):
            low = jnp.where(lane == j, now[j, :, :1], low)
            high = jnp.where(lane == j, now[j, :, rows - 1 :], high)
            ew_out[g, 0, j : j + 1] = now[j, :1]
            ew_out[g, 1, j : j + 1] = now[j, cols - 1 :]
        ns_out[g, 0] = low
        ns_out[g, 1] = high
        for side, (source, target, where) in enumerate(
            (
                (ew_out.at[g, 0], ew_in.at[g, 0], {"tile": west_t}),
                (ew_out.at[g, 1], ew_in.at[g, 1], {"tile": east_t}),
                (ns_out.at[g, 0], ns_in.at[g, 0], {"nest": low_n}),
                (ns_out.at[g, 1], ns_in.at[g, 1], {"nest": high_n}),
            )
        ):
            copy = remote(source, target, edge_send.at[g, side], edge_recv.at[g, side], where)
            copy.start()
            edges[g, side] = copy

    row_lane = lax.broadcasted_iota(jnp.int32, (cols, rows), 1)

    def finish(g):
        for side in range(4):
            edges[g, side].wait_recv()
        for j in range(per):
            f = g * per + j
            now = merged[f]
            east = jnp.concatenate([now[1:], ew_in[g, 0, j : j + 1]], axis=0)
            west = jnp.concatenate([ew_in[g, 1, j : j + 1], now[:-1]], axis=0)
            above = jnp.where(me_n == nests - 1, now[:, rows - 1 :], ns_in[g, 0, :, j : j + 1])
            below = jnp.where(me_n == 0, now[:, :1], ns_in[g, 1, :, j : j + 1])
            north = jnp.where(row_lane == rows - 1, above, pltpu.roll(now, rows - 1, 1))
            south = jnp.where(row_lane == 0, below, pltpu.roll(now, 1, 1))
            result[f] = now + rate_ref[f] * (east + west + north + south - 4.0 * now)

    first()
    lax.fori_loop(1, groups, restrict, 0)
    stages = {"F": forward, "P": relay, "M": merge, "E": finish}
    for step in order(groups):
        stages[step[0]](step[1])

    for g in range(groups):
        a2a_bytes(g).wait_send()
    for copy in [*sent.values(), *edges.values()]:
        copy.wait_send()


def per_device(
    child_fields, row_weights, col_weights, nest_offsets, priority, parent_old, smooth_rate
):
    planes, crow, ccols = child_fields.shape[1:]
    prd = row_weights.shape[0]
    _, cols, rows = parent_old.shape
    tiles, nests = lax.axis_size("tile"), lax.axis_size("nest")
    per = LANES // cols
    groups = planes // per
    nrows = prd * tiles
    hbm = pl.BlockSpec(memory_space=pl.ANY)
    dma = pltpu.SemaphoreType.DMA
    return pl.pallas_call(
        functools.partial(kernel, tiles, nests),
        out_shape=pltpu.VMEM(parent_old.shape, F32),
        in_specs=[hbm] * 7,
        out_specs=pl.BlockSpec(memory_space=pltpu.VMEM),
        scratch_shapes=[
            pltpu.SMEM((2, nests), jnp.int32),
            pltpu.SMEM((planes,), F32),
            pltpu.VMEM(row_weights.shape, F32),
            pltpu.VMEM((cols, rows), jnp.int32),
            pltpu.VMEM((planes, crow, ccols), F32),
            pltpu.VMEM(col_weights.shape, F32),
            pltpu.VMEM(col_weights.shape, BF16),
            pltpu.VMEM(col_weights.shape, BF16),
            pltpu.VMEM((2 * per * prd, ccols), BF16),
            pltpu.VMEM((per * prd, col_weights.shape[1]), F32),
            pltpu.VMEM((planes, cols, rows), F32),
            pltpu.VMEM((groups, tiles, prd, LANES), F32),
            pltpu.VMEM((groups, nrows, LANES), F32),
            pltpu.VMEM((groups, nrows // rows, LANES, rows), F32),
            pltpu.VMEM((groups, 2, LANES // 2, rows), F32),
            pltpu.VMEM((groups, 2, LANES // 2, rows), F32),
            pltpu.VMEM((groups, 2, LANES, rows), F32),
            pltpu.VMEM((2, cols, rows), jnp.int32),
            pltpu.VMEM((groups, 2, per, rows), F32),
            pltpu.VMEM((groups, 2, per, rows), F32),
            pltpu.VMEM((groups, 2, cols, LANES), F32),
            pltpu.VMEM((groups, 2, cols, LANES), F32),
            dma((4,)),
            dma((groups,)),
            dma((CHUNKS,)),
            dma,
            dma((groups,)),
            dma((groups,)),
            dma((2,)),
            dma((2,)),
            dma((groups, 2)),
            dma((groups, 2)),
            dma((groups, 4)),
            dma((groups, 4)),
            dma((groups, 4)),
            dma((groups, 4)),
        ],
        compiler_params=pltpu.CompilerParams(
            collective_id=0, has_side_effects=True, vmem_limit_bytes=60 * 2**20
        ),
    )(nest_offsets.T, smooth_rate, row_weights, priority, child_fields, col_weights, parent_old)


def solution(mesh):
    return jax.shard_map(
        per_device,
        mesh=mesh,
        in_specs=(
            P("nest", None, "tile", None),
            P(),
            P(),
            P(),
            P("tile", "nest"),
            P(None, "tile", "nest"),
            P(),
        ),
        out_specs=P(None, "tile", "nest"),
        check_vma=False,
    )
```

```python
import functools

import jax
import jax.numpy as jnp
from jax import lax
from jax.experimental import pallas as pl
from jax.experimental.pallas import tpu as pltpu
from jax.sharding import PartitionSpec as P

MESH = pl.DeviceIdType.MESH
LANES = 128
F32 = jnp.float32
BF16 = jnp.bfloat16
CHUNKS = 6
AHEAD = 3
SPAN = 2


def split(value):
    high = value.astype(BF16)
    return high, (value - high.astype(F32)).astype(BF16)


def dot(a, b):
    return jnp.dot(a, b, preferred_element_type=F32)


def remote(src, dst, send_sem, recv_sem, where):
    return pltpu.make_async_remote_copy(
        src_ref=src,
        dst_ref=dst,
        send_sem=send_sem,
        recv_sem=recv_sem,
        device_id=where,
        device_id_type=MESH,
    )


def order(groups):
    for g in range(groups + 1):
        if g < groups:
            yield "F", g
        if g > 0:
            yield "M", g - 1
        if g < groups:
            yield "P", g


def kernel(
    tiles,
    nests,
    offs_hbm,
    rate_hbm,
    rw_hbm,
    prio_hbm,
    child_hbm,
    cw_hbm,
    parent_hbm,
    result,
    offs_ref,
    rate_ref,
    rw_ref,
    prio_ref,
    child,
    cw,
    cw_high,
    cw_low,
    both_ref,
    restricted_ref,
    merged,
    pieces,
    strips,
    blocks,
    via,
    relayed,
    slabs,
    prio_near,
    ew_out,
    ew_old,
    ns_out,
    ns_old,
    ew_line,
    ew_cand,
    ns_cand,
    small_sem,
    child_sem,
    cw_sem,
    parent_sem,
    a2a_send,
    a2a_recv,
    near_send,
    near_recv,
    via_send,
    via_recv,
    slab_send,
    slab_recv,
    edge_send,
    edge_recv,
    ew_send,
    ew_recv,
    ns_send,
    ns_recv,
):
    planes, crow, ccols = child.shape
    prd = rw_ref.shape[0]
    cols, rows = prio_ref.shape
    per = LANES // cols
    groups = planes // per
    nrows = prd * tiles
    m = per * prd
    me_n, me_t = lax.axis_index("nest"), lax.axis_index("tile")

    def child_in(g):
        fields = pl.ds(g * per, per)
        return pltpu.make_async_copy(child_hbm.at[0, fields], child.at[fields], child_sem.at[g])

    chunks = cw_sem.shape[0]
    depth = ccols // chunks

    def cw_in(k):
        part = pl.ds(pl.multiple_of(k * depth, depth), depth)
        return pltpu.make_async_copy(cw_hbm.at[part], cw.at[part], cw_sem.at[k])

    parent_in = pltpu.make_async_copy(parent_hbm, merged, parent_sem)
    rw_in = pltpu.make_async_copy(rw_hbm, rw_ref, small_sem.at[0])
    prio_in = pltpu.make_async_copy(prio_hbm, prio_ref, small_sem.at[1])
    offs_in = pltpu.make_async_copy(offs_hbm, offs_ref, small_sem.at[2])
    rate_in = pltpu.make_async_copy(rate_hbm, rate_ref, small_sem.at[3])
    rw_in.start()
    child_in(0).start()
    for k in range(AHEAD):
        cw_in(k).start()
    offs_in.start()
    rate_in.start()
    prio_in.start()
    barrier = pltpu.get_barrier_semaphore()

    def greet_tile(d, carry):
        pl.semaphore_signal(
            barrier, inc=1, device_id={"tile": lax.rem(me_t + d, tiles)}, device_id_type=MESH
        )
        return carry

    lax.fori_loop(1, tiles, greet_tile, 0)
    for d in range(1, nests):
        there = lax.rem(me_n + d, nests)
        pl.semaphore_signal(barrier, inc=1, device_id={"nest": there}, device_id_type=MESH)
        for step in (1, tiles - 1):
            where = {"nest": there, "tile": lax.rem(me_t + step, tiles)}
            pl.semaphore_signal(barrier, inc=1, device_id=where, device_id_type=MESH)

    rw_in.wait()
    rw = rw_ref[...]
    spread_rows = lax.broadcasted_iota(jnp.int32, (per * crow, crow), 0)
    spread_cols = lax.broadcasted_iota(jnp.int32, (per * crow, crow), 1)
    spread = jnp.where(lax.rem(spread_rows, crow) == spread_cols, 1.0, 0.0).astype(BF16)
    wide_r = lax.broadcasted_iota(jnp.int32, (m, per * crow), 0)
    wide_c = lax.broadcasted_iota(jnp.int32, (m, per * crow), 1)
    diagonal = wide_r // prd == wide_c // crow
    block_rw = []
    for part in split(rw):
        line = lax.dot_general(
            part, spread, (((1,), (1,)), ((), ())), preferred_element_type=F32
        )
        line = jnp.concatenate([line] * per, axis=0)
        block_rw.append(jnp.where(diagonal, line, 0.0).astype(BF16))
    both_rw = jnp.concatenate(block_rw, axis=0)

    lane_group = lax.broadcasted_iota(jnp.int32, (prd, LANES), 1) // cols
    offs_in.wait()
    rate_in.wait()
    left, top = jnp.int32(0), jnp.int32(0)
    for n in range(nests):
        left = jnp.where(me_n == n, offs_ref[1, n], left)
        top = jnp.where(me_n == n, offs_ref[0, n], top)
    top = lax.rem(top, nrows)

    here = pl.ds(pl.multiple_of(me_t * prd, prd), prd)

    def fold(both, high, b_high, b_low):
        wide = dot(both, b_high)
        return (wide[:m] + wide[m:]) + dot(high, b_low)

    def thin(g):
        block = child[pl.ds(g * per, per)].reshape(per * crow, ccols)
        thinned = fold(both_rw, block_rw[0], *split(block))
        high, low = split(thinned)
        both_ref[:m] = high
        both_ref[m:] = low

    def cut(g):
        restricted = pltpu.roll(restricted_ref[...], left, 1)
        for base in range(0, tiles * cols, LANES):
            parts = [restricted[j * prd : (j + 1) * prd, base : base + LANES] for j in range(per)]
            step = per // 2
            while step:
                for a in range(per):
                    if a & step:
                        continue
                    one, two = parts[a], parts[a + step]
                    keep = lane_group & step == 0
                    parts[a] = jnp.where(keep, one, pltpu.roll(two, step * cols, 1))
                    parts[a + step] = jnp.where(keep, pltpu.roll(one, LANES - step * cols, 1), two)
                step //= 2
            for q in range(per):
                pieces[g, base // cols + q] = parts[q]
        strips[g, here, :] = pieces[g, me_t]

    def send(g):
        def send_one(d, carry):
            t = lax.rem(me_t + d, tiles)
            remote(
                pieces.at[g, t],
                strips.at[g, here, :],
                a2a_send.at[g],
                a2a_recv.at[g],
                {"tile": t},
            ).start()
            return carry

        lax.fori_loop(1, tiles, send_one, 0)

    def first():
        child_in(0).wait()
        cw_in(AHEAD).start()
        thin(0)
        for k in range(0, chunks, SPAN):
            part = slice(k * depth, (k + SPAN) * depth)
            for c in range(k, k + SPAN):
                cw_in(c).wait()
                if c + AHEAD + 1 < chunks:
                    cw_in(c + AHEAD + 1).start()
                for g in range(1, groups):
                    if c == min(chunks - AHEAD - 2 + g, chunks - 1):
                        child_in(g).start()
            w_high, w_low = split(cw[part])
            cw_high[part] = w_high
            cw_low[part] = w_low
            now = fold(both_ref[:, part], both_ref[:m, part], w_high, w_low)
            restricted_ref[...] = now if k == 0 else restricted_ref[...] + now
        cut(0)
        parent_in.start()
        pl.semaphore_wait(barrier, tiles - 1 + 3 * (nests - 1))
        swap_priorities()
        send(0)

    def restrict(g, carry):
        child_in(g).wait()
        thin(g)
        restricted_ref[...] = fold(both_ref[...], both_ref[:m], cw_high[...], cw_low[...])
        cut(g)
        send(g)
        return carry

    def a2a_bytes(g):
        most = strips.at[g, pl.ds(0, prd * (tiles - 1)), :]
        return remote(most, most, a2a_send.at[g], a2a_recv.at[g], {"tile": me_t})

    prio_in.wait()
    prio = prio_ref[...]
    west_t, east_t = lax.rem(me_t + tiles - 1, tiles), lax.rem(me_t + 1, tiles)
    low_n, high_n = lax.rem(me_n + nests - 1, nests), lax.rem(me_n + 1, nests)
    lane = lax.broadcasted_iota(jnp.int32, (cols, LANES), 1)

    near = lax.rem(me_n + 1, 2)
    half = LANES // 2
    halves = pl.ds(0, half), pl.ds(half, half)
    sent = {}

    def pass_on(key, source, target, sems, to, tile=None):
        where = {"nest": to} if tile is None else {"nest": to, "tile": tile}
        copy = remote(source, target, *sems, where)
        copy.start()
        sent[key] = copy

    def swap_priorities():
        for side, to in enumerate((high_n, low_n)):
            sems = near_send.at[side], near_recv.at[side]
            pass_on(("prio", side), prio_ref, prio_near.at[side], sems, to)

    strip_row = lax.broadcasted_iota(jnp.int32, (nrows, LANES), 0)

    def forward(g):
        a2a_bytes(g).wait_recv()
        turned = pltpu.roll(strips[g].T, top, 1)
        for b in range(nrows // rows):
            blocks[g, b] = turned[:, b * rows : (b + 1) * rows]
        for side, to in enumerate((high_n, low_n)):
            source = blocks.at[g, 1 - near, halves[side]]
            sems = via_send.at[g, side], via_recv.at[g, side]
            pass_on(("via", g, side), source, via.at[g, side], sems, to)
        for side, to in enumerate((high_n, low_n)):
            part = halves[1 - side]
            sems = slab_send.at[g, side], slab_recv.at[g, side]
            source = blocks.at[g, near, part]
            pass_on(("slab", g, side), source, slabs.at[g, side, part], sems, to)
        for side, col in enumerate((0, cols - 1)):
            for j in range(per):
                at = j * cols + col
                for b in range(nrows // rows):
                    ew_line[g, side, b, j : j + 1] = turned[at : at + 1, b * rows : (b + 1) * rows]
        for q, residue in enumerate((nrows - 1, rows, rows - 1, 0)):
            picked = strip_row == lax.rem(residue + nrows - top, nrows)
            line = jnp.sum(jnp.where(picked, strips[g], 0.0), axis=0, keepdims=True)
            ns_cand[g, q : q + 1] = line
            ns_cand[g, q + 4 : q + 5] = line
        for d in range(nests):
            to = lax.rem(me_n + d, nests)
            for side, tile in enumerate((west_t, east_t)):
                source = ew_line.at[g, side, lax.rem(to, 2)]
                sems = ew_send.at[g, side, d], ew_recv.at[g, side, d]
                pass_on(("ew", g, side, d), source, ew_cand.at[g, side, d], sems, to, tile)
            if d:
                source, target = ns_cand.at[g, pl.ds(0, 8)], ns_cand.at[g, pl.ds(d * 8, 8)]
                sems = ns_send.at[g, d - 1], ns_recv.at[g, d - 1]
                pass_on(("ns", g, d), source, target, sems, to)

    def relay(g):
        if g == 0:
            for side in range(2):
                sent["prio", side].wait_recv()
        for side, to in enumerate((high_n, low_n)):
            sent["via", g, side].wait_recv()
            origin = (low_n, high_n)[side]
            theirs = (prio_near[1 - side] == origin)[None]
            far = via[g, side].reshape(per // 2, cols, rows)
            own = blocks[g, near, side * half : (side + 1) * half].reshape(per // 2, cols, rows)
            relayed[g, side] = jnp.where(theirs, far, own).reshape(half, rows)
            sems = slab_send.at[g, 2 + side], slab_recv.at[g, 2 + side]
            target = slabs.at[g, side, halves[side]]
            pass_on(("slab", g, 2 + side), relayed.at[g, side], target, sems, to)

    row_lane = lax.broadcasted_iota(jnp.int32, (cols, rows), 1)

    def swap_edges():
        parent_in.wait()
        prio_f = prio.astype(F32)
        for side, row in enumerate((0, rows - 1)):
            line = jnp.zeros((cols, LANES), F32)
            for f in range(planes):
                line = jnp.where(lane == f, merged[f, :, row : row + 1], line)
            ns_out[side] = jnp.where(lane == planes, prio_f[:, row : row + 1], line)
            sems = edge_send.at[side], edge_recv.at[side]
            to = (low_n, high_n)[side]
            pass_on(("old", side), ns_out.at[side], ns_old.at[side], sems, to)
        for side, col in enumerate((0, cols - 1)):
            for f in range(planes):
                ew_out[side, f : f + 1] = merged[f, col : col + 1]
            ew_out[side, planes:] = jnp.broadcast_to(prio_f[col : col + 1], (8, rows))
            sems = edge_send.at[2 + side], edge_recv.at[2 + side]
            tile = (west_t, east_t)[side]
            pass_on(("old", 2 + side), ew_out.at[side], ew_old.at[side], sems, me_n, tile)

    def merge(g):
        if g == 0:
            for side in range(4):
                sent["old", side].wait_recv()
        now = merged[g * per : (g + 1) * per]
        mine = blocks[g, 1 - near].reshape(per, cols, rows)
        now = jnp.where((prio == me_n)[None], mine, now)
        for q in range(4):
            sent["slab", g, q].wait_recv()
        far_n = lax.rem(me_n + 2, nests)
        ways = [(prio == n)[None] for n in (low_n, high_n)]
        far = (prio == far_n)[None]
        mixed = []
        for side in range(2):
            part = now[side * (per // 2) : (side + 1) * (per // 2)]
            for way in range(2):
                take = (ways[way] | far) if way == side else ways[way]
                slab = slabs[g, way, side * half : (side + 1) * half]
                part = jnp.where(take, slab.reshape(per // 2, cols, rows), part)
            mixed.append(part)
        now = jnp.concatenate(mixed, axis=0)
        origins = [lax.rem(me_n + nests - d, nests).astype(F32) for d in range(nests)]
        beside = []
        for side in range(2):
            line = ew_old[side, g * per : (g + 1) * per]
            owner = ew_old[side, planes:]
            for d in range(nests):
                sent["ew", g, side, d].wait_recv()
                line = jnp.where(owner == origins[d], ew_cand[g, side, d], line)
            beside.append(line)
        for d in range(1, nests):
            sent["ns", g, d].wait_recv()
        lines = [
            ns_cand[g, pl.ds(d * 8 + 2 * (1 - near) + way, 1), :]
            for way in range(2)
            for d in range(nests)
        ]
        lines.append(jnp.zeros((LANES - 2 * nests, LANES), F32))
        ends = jnp.concatenate(lines, axis=0).T
        for j in range(per):
            f = g * per + j
            here_j = now[j]
            outer = []
            for way in range(2):
                old = ns_old[1 - way]
                cell, owner = old[:, f : f + 1], old[:, planes : planes + 1]
                for d in range(nests):
                    at = way * nests + d
                    new = ends[j * cols : (j + 1) * cols, at : at + 1]
                    cell = jnp.where(owner == origins[d], new, cell)
                outer.append(cell)
            east = jnp.concatenate([here_j[1:], beside[0][j : j + 1]], axis=0)
            west = jnp.concatenate([beside[1][j : j + 1], here_j[:-1]], axis=0)
            above = jnp.where(me_n == nests - 1, here_j[:, rows - 1 :], outer[1])
            below = jnp.where(me_n == 0, here_j[:, :1], outer[0])
            north = jnp.where(row_lane == rows - 1, above, pltpu.roll(here_j, rows - 1, 1))
            south = jnp.where(row_lane == 0, below, pltpu.roll(here_j, 1, 1))
            result[f] = here_j + rate_ref[f] * (east + west + north + south - 4.0 * here_j)

    first()
    lax.fori_loop(1, groups, restrict, 0)
    swap_edges()
    stages = {"F": forward, "P": relay, "M": merge}
    for step in order(groups):
        stages[step[0]](step[1])

    for g in range(groups):
        a2a_bytes(g).wait_send()
    for copy in sent.values():
        copy.wait_send()


def per_device(
    child_fields, row_weights, col_weights, nest_offsets, priority, parent_old, smooth_rate
):
    planes, crow, ccols = child_fields.shape[1:]
    prd = row_weights.shape[0]
    _, cols, rows = parent_old.shape
    tiles, nests = lax.axis_size("tile"), lax.axis_size("nest")
    per = LANES // cols
    groups = planes // per
    nrows = prd * tiles
    hbm = pl.BlockSpec(memory_space=pl.ANY)
    dma = pltpu.SemaphoreType.DMA
    return pl.pallas_call(
        functools.partial(kernel, tiles, nests),
        out_shape=pltpu.VMEM(parent_old.shape, F32),
        in_specs=[hbm] * 7,
        out_specs=pl.BlockSpec(memory_space=pltpu.VMEM),
        scratch_shapes=[
            pltpu.SMEM((2, nests), jnp.int32),
            pltpu.SMEM((planes,), F32),
            pltpu.VMEM(row_weights.shape, F32),
            pltpu.VMEM((cols, rows), jnp.int32),
            pltpu.VMEM((planes, crow, ccols), F32),
            pltpu.VMEM(col_weights.shape, F32),
            pltpu.VMEM(col_weights.shape, BF16),
            pltpu.VMEM(col_weights.shape, BF16),
            pltpu.VMEM((2 * per * prd, ccols), BF16),
            pltpu.VMEM((per * prd, col_weights.shape[1]), F32),
            pltpu.VMEM((planes, cols, rows), F32),
            pltpu.VMEM((groups, tiles, prd, LANES), F32),
            pltpu.VMEM((groups, nrows, LANES), F32),
            pltpu.VMEM((groups, nrows // rows, LANES, rows), F32),
            pltpu.VMEM((groups, 2, LANES // 2, rows), F32),
            pltpu.VMEM((groups, 2, LANES // 2, rows), F32),
            pltpu.VMEM((groups, 2, LANES, rows), F32),
            pltpu.VMEM((2, cols, rows), jnp.int32),
            pltpu.VMEM((2, planes + 8, rows), F32),
            pltpu.VMEM((2, planes + 8, rows), F32),
            pltpu.VMEM((2, cols, LANES), F32),
            pltpu.VMEM((2, cols, LANES), F32),
            pltpu.VMEM((groups, 2, nrows // rows, per, rows), F32),
            pltpu.VMEM((groups, 2, nests, per, rows), F32),
            pltpu.VMEM((groups, 8 * nests, LANES), F32),
            dma((4,)),
            dma((groups,)),
            dma((CHUNKS,)),
            dma,
            dma((groups,)),
            dma((groups,)),
            dma((2,)),
            dma((2,)),
            dma((groups, 2)),
            dma((groups, 2)),
            dma((groups, 4)),
            dma((groups, 4)),
            dma((4,)),
            dma((4,)),
            dma((groups, 2, nests)),
            dma((groups, 2, nests)),
            dma((groups, nests - 1)),
            dma((groups, nests - 1)),
        ],
        compiler_params=pltpu.CompilerParams(
            collective_id=0, has_side_effects=True, vmem_limit_bytes=60 * 2**20
        ),
    )(nest_offsets.T, smooth_rate, row_weights, priority, child_fields, col_weights, parent_old)


def solution(mesh):
    return jax.shard_map(
        per_device,
        mesh=mesh,
        in_specs=(
            P("nest", None, "tile", None),
            P(),
            P(),
            P(),
            P("tile", "nest"),
            P(None, "tile", "nest"),
            P(),
        ),
        out_specs=P(None, "tile", "nest"),
        check_vma=False,
    )
```

```python
import functools

import jax
import jax.numpy as jnp
from jax import lax
from jax.experimental import pallas as pl
from jax.experimental.pallas import tpu as pltpu
from jax.sharding import PartitionSpec as P

MESH = pl.DeviceIdType.MESH
LANES = 128
F32 = jnp.float32
BF16 = jnp.bfloat16
CHUNKS = 6
AHEAD = 3
SPAN = 2


def split(value):
    high = value.astype(BF16)
    return high, (value - high.astype(F32)).astype(BF16)


def dot(a, b):
    return jnp.dot(a, b, preferred_element_type=F32)


def remote(src, dst, send_sem, recv_sem, where):
    return pltpu.make_async_remote_copy(
        src_ref=src,
        dst_ref=dst,
        send_sem=send_sem,
        recv_sem=recv_sem,
        device_id=where,
        device_id_type=MESH,
    )


def order(groups):
    for g in range(groups):
        yield "F", g
        yield "P", g
    for g in range(groups):
        yield "M", g


def kernel(
    tiles,
    nests,
    offs_hbm,
    rate_hbm,
    rw_hbm,
    prio_hbm,
    child_hbm,
    cw_hbm,
    parent_hbm,
    result,
    offs_ref,
    rate_ref,
    rw_ref,
    prio_ref,
    child,
    cw,
    cw_high,
    cw_low,
    both_ref,
    restricted_ref,
    merged,
    pieces,
    strips,
    blocks,
    via,
    relayed,
    slabs,
    prio_near,
    ew_out,
    ew_old,
    ns_out,
    ns_old,
    ew_line,
    ew_cand,
    ns_cand,
    small_sem,
    child_sem,
    cw_sem,
    parent_sem,
    a2a_send,
    a2a_recv,
    near_send,
    near_recv,
    via_send,
    via_recv,
    slab_send,
    slab_recv,
    edge_send,
    edge_recv,
    ew_send,
    ew_recv,
    ns_send,
    ns_recv,
):
    planes, crow, ccols = child.shape
    prd = rw_ref.shape[0]
    cols, rows = prio_ref.shape
    per = LANES // cols
    groups = planes // per
    nrows = prd * tiles
    m = per * prd
    me_n, me_t = lax.axis_index("nest"), lax.axis_index("tile")

    def child_in(g):
        fields = pl.ds(g * per, per)
        return pltpu.make_async_copy(child_hbm.at[0, fields], child.at[fields], child_sem.at[g])

    chunks = cw_sem.shape[0]
    depth = ccols // chunks

    def cw_in(k):
        part = pl.ds(pl.multiple_of(k * depth, depth), depth)
        return pltpu.make_async_copy(cw_hbm.at[part], cw.at[part], cw_sem.at[k])

    parent_in = pltpu.make_async_copy(parent_hbm, merged, parent_sem)
    rw_in = pltpu.make_async_copy(rw_hbm, rw_ref, small_sem.at[0])
    prio_in = pltpu.make_async_copy(prio_hbm, prio_ref, small_sem.at[1])
    offs_in = pltpu.make_async_copy(offs_hbm, offs_ref, small_sem.at[2])
    rate_in = pltpu.make_async_copy(rate_hbm, rate_ref, small_sem.at[3])
    rw_in.start()
    child_in(0).start()
    for k in range(AHEAD):
        cw_in(k).start()
    offs_in.start()
    rate_in.start()
    prio_in.start()
    barrier = pltpu.get_barrier_semaphore()

    def greet_tile(d, carry):
        pl.semaphore_signal(
            barrier, inc=1, device_id={"tile": lax.rem(me_t + d, tiles)}, device_id_type=MESH
        )
        return carry

    lax.fori_loop(1, tiles, greet_tile, 0)
    for d in range(1, nests):
        there = lax.rem(me_n + d, nests)
        pl.semaphore_signal(barrier, inc=1, device_id={"nest": there}, device_id_type=MESH)
        for step in (1, tiles - 1):
            where = {"nest": there, "tile": lax.rem(me_t + step, tiles)}
            pl.semaphore_signal(barrier, inc=1, device_id=where, device_id_type=MESH)

    rw_in.wait()
    rw = rw_ref[...]
    spread_rows = lax.broadcasted_iota(jnp.int32, (per * crow, crow), 0)
    spread_cols = lax.broadcasted_iota(jnp.int32, (per * crow, crow), 1)
    spread = jnp.where(lax.rem(spread_rows, crow) == spread_cols, 1.0, 0.0).astype(BF16)
    wide_r = lax.broadcasted_iota(jnp.int32, (m, per * crow), 0)
    wide_c = lax.broadcasted_iota(jnp.int32, (m, per * crow), 1)
    diagonal = wide_r // prd == wide_c // crow
    block_rw = []
    for part in split(rw):
        line = lax.dot_general(
            part, spread, (((1,), (1,)), ((), ())), preferred_element_type=F32
        )
        line = jnp.concatenate([line] * per, axis=0)
        block_rw.append(jnp.where(diagonal, line, 0.0).astype(BF16))
    both_rw = jnp.concatenate(block_rw, axis=0)

    lane_group = lax.broadcasted_iota(jnp.int32, (prd, LANES), 1) // cols
    offs_in.wait()
    rate_in.wait()
    left, top = jnp.int32(0), jnp.int32(0)
    for n in range(nests):
        left = jnp.where(me_n == n, offs_ref[1, n], left)
        top = jnp.where(me_n == n, offs_ref[0, n], top)
    top = lax.rem(top, nrows)

    here = pl.ds(pl.multiple_of(me_t * prd, prd), prd)

    def fold(both, high, b_high, b_low):
        wide = dot(both, b_high)
        return (wide[:m] + wide[m:]) + dot(high, b_low)

    def thin(g):
        block = child[pl.ds(g * per, per)].reshape(per * crow, ccols)
        thinned = fold(both_rw, block_rw[0], *split(block))
        high, low = split(thinned)
        both_ref[:m] = high
        both_ref[m:] = low

    def cut(g):
        restricted = pltpu.roll(restricted_ref[...], left, 1)
        for base in range(0, tiles * cols, LANES):
            parts = [restricted[j * prd : (j + 1) * prd, base : base + LANES] for j in range(per)]
            step = per // 2
            while step:
                for a in range(per):
                    if a & step:
                        continue
                    one, two = parts[a], parts[a + step]
                    keep = lane_group & step == 0
                    parts[a] = jnp.where(keep, one, pltpu.roll(two, step * cols, 1))
                    parts[a + step] = jnp.where(keep, pltpu.roll(one, LANES - step * cols, 1), two)
                step //= 2
            for q in range(per):
                pieces[g, base // cols + q] = parts[q]
        strips[g, here, :] = pieces[g, me_t]

    def send(g):
        def send_one(d, carry):
            t = lax.rem(me_t + d, tiles)
            remote(
                pieces.at[g, t],
                strips.at[g, here, :],
                a2a_send.at[g],
                a2a_recv.at[g],
                {"tile": t},
            ).start()
            return carry

        lax.fori_loop(1, tiles, send_one, 0)

    def first():
        child_in(0).wait()
        cw_in(AHEAD).start()
        thin(0)
        for k in range(0, chunks, SPAN):
            part = slice(k * depth, (k + SPAN) * depth)
            for c in range(k, k + SPAN):
                cw_in(c).wait()
                if c + AHEAD + 1 < chunks:
                    cw_in(c + AHEAD + 1).start()
                for g in range(1, groups):
                    if c == min(chunks - AHEAD - 2 + g, chunks - 1):
                        child_in(g).start()
            w_high, w_low = split(cw[part])
            cw_high[part] = w_high
            cw_low[part] = w_low
            now = fold(both_ref[:, part], both_ref[:m, part], w_high, w_low)
            restricted_ref[...] = now if k == 0 else restricted_ref[...] + now
        cut(0)
        parent_in.start()
        pl.semaphore_wait(barrier, tiles - 1 + 3 * (nests - 1))
        swap_priorities()
        send(0)

    def restrict(g, carry):
        child_in(g).wait()
        thin(g)
        restricted_ref[...] = fold(both_ref[...], both_ref[:m], cw_high[...], cw_low[...])
        cut(g)
        send(g)
        return carry

    def a2a_bytes(g):
        most = strips.at[g, pl.ds(0, prd * (tiles - 1)), :]
        return remote(most, most, a2a_send.at[g], a2a_recv.at[g], {"tile": me_t})

    prio_in.wait()
    prio = prio_ref[...]
    west_t, east_t = lax.rem(me_t + tiles - 1, tiles), lax.rem(me_t + 1, tiles)
    low_n, high_n = lax.rem(me_n + nests - 1, nests), lax.rem(me_n + 1, nests)
    lane = lax.broadcasted_iota(jnp.int32, (cols, LANES), 1)

    near = lax.rem(me_n + 1, 2)
    half = LANES // 2
    halves = pl.ds(0, half), pl.ds(half, half)
    sent = {}

    def pass_on(key, source, target, sems, to, tile=None):
        where = {"nest": to} if tile is None else {"nest": to, "tile": tile}
        copy = remote(source, target, *sems, where)
        copy.start()
        sent[key] = copy

    def swap_priorities():
        for side, to in enumerate((high_n, low_n)):
            sems = near_send.at[side], near_recv.at[side]
            pass_on(("prio", side), prio_ref, prio_near.at[side], sems, to)

    strip_row = lax.broadcasted_iota(jnp.int32, (nrows, LANES), 0)

    def forward(g):
        a2a_bytes(g).wait_recv()
        turned = pltpu.roll(strips[g].T, top, 1)
        for b in range(nrows // rows):
            blocks[g, b] = turned[:, b * rows : (b + 1) * rows]
        for side, to in enumerate((high_n, low_n)):
            source = blocks.at[g, 1 - near, halves[side]]
            sems = via_send.at[g, side], via_recv.at[g, side]
            pass_on(("via", g, side), source, via.at[g, side], sems, to)
        for side, to in enumerate((high_n, low_n)):
            part = halves[1 - side]
            sems = slab_send.at[g, side], slab_recv.at[g, side]
            source = blocks.at[g, near, part]
            pass_on(("slab", g, side), source, slabs.at[g, side, part], sems, to)
        for side, col in enumerate((0, cols - 1)):
            for j in range(per):
                at = j * cols + col
                for b in range(nrows // rows):
                    ew_line[g, side, b, j : j + 1] = turned[at : at + 1, b * rows : (b + 1) * rows]
        for q, residue in enumerate((nrows - 1, rows, rows - 1, 0)):
            picked = strip_row == lax.rem(residue + nrows - top, nrows)
            line = jnp.sum(jnp.where(picked, strips[g], 0.0), axis=0, keepdims=True)
            ns_cand[g, q : q + 1] = line
            ns_cand[g, q + 4 : q + 5] = line
        for d in range(nests):
            to = lax.rem(me_n + d, nests)
            for side, tile in enumerate((west_t, east_t)):
                source = ew_line.at[g, side, lax.rem(to, 2)]
                sems = ew_send.at[g, side, d], ew_recv.at[g, side, d]
                pass_on(("ew", g, side, d), source, ew_cand.at[g, side, d], sems, to, tile)
            if d:
                source, target = ns_cand.at[g, pl.ds(0, 8)], ns_cand.at[g, pl.ds(d * 8, 8)]
                sems = ns_send.at[g, d - 1], ns_recv.at[g, d - 1]
                pass_on(("ns", g, d), source, target, sems, to)

    def relay(g):
        if g == 0:
            for side in range(2):
                sent["prio", side].wait_recv()
        for side, to in enumerate((high_n, low_n)):
            sent["via", g, side].wait_recv()
            origin = (low_n, high_n)[side]
            theirs = (prio_near[1 - side] == origin)[None]
            far = via[g, side].reshape(per // 2, cols, rows)
            own = blocks[g, near, side * half : (side + 1) * half].reshape(per // 2, cols, rows)
            relayed[g, side] = jnp.where(theirs, far, own).reshape(half, rows)
            sems = slab_send.at[g, 2 + side], slab_recv.at[g, 2 + side]
            target = slabs.at[g, side, halves[side]]
            pass_on(("slab", g, 2 + side), relayed.at[g, side], target, sems, to)

    row_lane = lax.broadcasted_iota(jnp.int32, (cols, rows), 1)

    def swap_edges():
        parent_in.wait()
        prio_f = prio.astype(F32)
        for side, row in enumerate((0, rows - 1)):
            line = jnp.zeros((cols, LANES), F32)
            for f in range(planes):
                line = jnp.where(lane == f, merged[f, :, row : row + 1], line)
            ns_out[side] = jnp.where(lane == planes, prio_f[:, row : row + 1], line)
            sems = edge_send.at[side], edge_recv.at[side]
            to = (low_n, high_n)[side]
            pass_on(("old", side), ns_out.at[side], ns_old.at[side], sems, to)
        for side, col in enumerate((0, cols - 1)):
            for f in range(planes):
                ew_out[side, f : f + 1] = merged[f, col : col + 1]
            ew_out[side, planes:] = jnp.broadcast_to(prio_f[col : col + 1], (8, rows))
            sems = edge_send.at[2 + side], edge_recv.at[2 + side]
            tile = (west_t, east_t)[side]
            pass_on(("old", 2 + side), ew_out.at[side], ew_old.at[side], sems, me_n, tile)

    def merge(g):
        if g == 0:
            for side in range(4):
                sent["old", side].wait_recv()
        now = merged[g * per : (g + 1) * per]
        mine = blocks[g, 1 - near].reshape(per, cols, rows)
        now = jnp.where((prio == me_n)[None], mine, now)
        for q in range(4):
            sent["slab", g, q].wait_recv()
        far_n = lax.rem(me_n + 2, nests)
        ways = [(prio == n)[None] for n in (low_n, high_n)]
        far = (prio == far_n)[None]
        mixed = []
        for side in range(2):
            part = now[side * (per // 2) : (side + 1) * (per // 2)]
            for way in range(2):
                take = (ways[way] | far) if way == side else ways[way]
                slab = slabs[g, way, side * half : (side + 1) * half]
                part = jnp.where(take, slab.reshape(per // 2, cols, rows), part)
            mixed.append(part)
        now = jnp.concatenate(mixed, axis=0)
        origins = [lax.rem(me_n + nests - d, nests).astype(F32) for d in range(nests)]
        beside = []
        for side in range(2):
            line = ew_old[side, g * per : (g + 1) * per]
            owner = ew_old[side, planes:]
            for d in range(nests):
                sent["ew", g, side, d].wait_recv()
                line = jnp.where(owner == origins[d], ew_cand[g, side, d], line)
            beside.append(line)
        for d in range(1, nests):
            sent["ns", g, d].wait_recv()
        lines = [
            ns_cand[g, pl.ds(d * 8 + 2 * (1 - near) + way, 1), :]
            for way in range(2)
            for d in range(nests)
        ]
        lines.append(jnp.zeros((LANES - 2 * nests, LANES), F32))
        ends = jnp.concatenate(lines, axis=0).T
        for j in range(per):
            f = g * per + j
            here_j = now[j]
            outer = []
            for way in range(2):
                old = ns_old[1 - way]
                cell, owner = old[:, f : f + 1], old[:, planes : planes + 1]
                for d in range(nests):
                    at = way * nests + d
                    new = ends[j * cols : (j + 1) * cols, at : at + 1]
                    cell = jnp.where(owner == origins[d], new, cell)
                outer.append(cell)
            east = jnp.concatenate([here_j[1:], beside[0][j : j + 1]], axis=0)
            west = jnp.concatenate([beside[1][j : j + 1], here_j[:-1]], axis=0)
            above = jnp.where(me_n == nests - 1, here_j[:, rows - 1 :], outer[1])
            below = jnp.where(me_n == 0, here_j[:, :1], outer[0])
            north = jnp.where(row_lane == rows - 1, above, pltpu.roll(here_j, rows - 1, 1))
            south = jnp.where(row_lane == 0, below, pltpu.roll(here_j, 1, 1))
            result[f] = here_j + rate_ref[f] * (east + west + north + south - 4.0 * here_j)

    first()
    lax.fori_loop(1, groups, restrict, 0)
    swap_edges()
    stages = {"F": forward, "P": relay, "M": merge}
    for step in order(groups):
        stages[step[0]](step[1])

    for g in range(groups):
        a2a_bytes(g).wait_send()
    for copy in sent.values():
        copy.wait_send()


def per_device(
    child_fields, row_weights, col_weights, nest_offsets, priority, parent_old, smooth_rate
):
    planes, crow, ccols = child_fields.shape[1:]
    prd = row_weights.shape[0]
    _, cols, rows = parent_old.shape
    tiles, nests = lax.axis_size("tile"), lax.axis_size("nest")
    per = LANES // cols
    groups = planes // per
    nrows = prd * tiles
    hbm = pl.BlockSpec(memory_space=pl.ANY)
    dma = pltpu.SemaphoreType.DMA
    return pl.pallas_call(
        functools.partial(kernel, tiles, nests),
        out_shape=pltpu.VMEM(parent_old.shape, F32),
        in_specs=[hbm] * 7,
        out_specs=pl.BlockSpec(memory_space=pltpu.VMEM),
        scratch_shapes=[
            pltpu.SMEM((2, nests), jnp.int32),
            pltpu.SMEM((planes,), F32),
            pltpu.VMEM(row_weights.shape, F32),
            pltpu.VMEM((cols, rows), jnp.int32),
            pltpu.VMEM((planes, crow, ccols), F32),
            pltpu.VMEM(col_weights.shape, F32),
            pltpu.VMEM(col_weights.shape, BF16),
            pltpu.VMEM(col_weights.shape, BF16),
            pltpu.VMEM((2 * per * prd, ccols), BF16),
            pltpu.VMEM((per * prd, col_weights.shape[1]), F32),
            pltpu.VMEM((planes, cols, rows), F32),
            pltpu.VMEM((groups, tiles, prd, LANES), F32),
            pltpu.VMEM((groups, nrows, LANES), F32),
            pltpu.VMEM((groups, nrows // rows, LANES, rows), F32),
            pltpu.VMEM((groups, 2, LANES // 2, rows), F32),
            pltpu.VMEM((groups, 2, LANES // 2, rows), F32),
            pltpu.VMEM((groups, 2, LANES, rows), F32),
            pltpu.VMEM((2, cols, rows), jnp.int32),
            pltpu.VMEM((2, planes + 8, rows), F32),
            pltpu.VMEM((2, planes + 8, rows), F32),
            pltpu.VMEM((2, cols, LANES), F32),
            pltpu.VMEM((2, cols, LANES), F32),
            pltpu.VMEM((groups, 2, nrows // rows, per, rows), F32),
            pltpu.VMEM((groups, 2, nests, per, rows), F32),
            pltpu.VMEM((groups, 8 * nests, LANES), F32),
            dma((4,)),
            dma((groups,)),
            dma((CHUNKS,)),
            dma,
            dma((groups,)),
            dma((groups,)),
            dma((2,)),
            dma((2,)),
            dma((groups, 2)),
            dma((groups, 2)),
            dma((groups, 4)),
            dma((groups, 4)),
            dma((4,)),
            dma((4,)),
            dma((groups, 2, nests)),
            dma((groups, 2, nests)),
            dma((groups, nests - 1)),
            dma((groups, nests - 1)),
        ],
        compiler_params=pltpu.CompilerParams(
            collective_id=0, has_side_effects=True, vmem_limit_bytes=60 * 2**20
        ),
    )(nest_offsets.T, smooth_rate, row_weights, priority, child_fields, col_weights, parent_old)


def solution(mesh):
    return jax.shard_map(
        per_device,
        mesh=mesh,
        in_specs=(
            P("nest", None, "tile", None),
            P(),
            P(),
            P(),
            P("tile", "nest"),
            P(None, "tile", "nest"),
            P(),
        ),
        out_specs=P(None, "tile", "nest"),
        check_vma=False,
    )
```

```python
import functools

import jax
import jax.numpy as jnp
from jax import lax
from jax.experimental import pallas as pl
from jax.experimental.pallas import tpu as pltpu
from jax.sharding import PartitionSpec as P

MESH = pl.DeviceIdType.MESH
LANES = 128
F32 = jnp.float32
BF16 = jnp.bfloat16
CHUNKS = 6
AHEAD = 3
SPAN = 2


def split(value):
    high = value.astype(BF16)
    return high, (value - high.astype(F32)).astype(BF16)


def dot(a, b):
    return jnp.dot(a, b, preferred_element_type=F32)


def remote(src, dst, send_sem, recv_sem, where):
    return pltpu.make_async_remote_copy(
        src_ref=src,
        dst_ref=dst,
        send_sem=send_sem,
        recv_sem=recv_sem,
        device_id=where,
        device_id_type=MESH,
    )


def order(groups):
    for g in range(groups):
        yield "F", g
        yield "P", g
    for g in range(groups):
        yield "M", g


def kernel(
    tiles,
    nests,
    offs_hbm,
    rate_hbm,
    rw_hbm,
    prio_hbm,
    child_hbm,
    cw_hbm,
    parent_hbm,
    result,
    offs_ref,
    rate_ref,
    rw_ref,
    prio_ref,
    child,
    cw,
    cw_high,
    cw_low,
    both_ref,
    restricted_ref,
    merged,
    pieces,
    strips,
    blocks,
    via,
    relayed,
    slabs,
    prio_near,
    ew_out,
    ew_old,
    ns_out,
    ns_old,
    ew_line,
    ew_cand,
    ns_cand,
    small_sem,
    child_sem,
    cw_sem,
    parent_sem,
    a2a_send,
    a2a_recv,
    near_send,
    near_recv,
    via_send,
    via_recv,
    slab_send,
    slab_recv,
    edge_send,
    edge_recv,
    ew_send,
    ew_recv,
    ns_send,
    ns_recv,
):
    planes, crow, ccols = child.shape
    prd = rw_ref.shape[0]
    cols, rows = prio_ref.shape
    per = LANES // cols
    groups = planes // per
    nrows = prd * tiles
    m = per * prd
    me_n, me_t = lax.axis_index("nest"), lax.axis_index("tile")

    def child_in(g):
        fields = pl.ds(g * per, per)
        return pltpu.make_async_copy(child_hbm.at[0, fields], child.at[fields], child_sem.at[g])

    chunks = cw_sem.shape[0]
    depth = ccols // chunks

    def cw_in(k):
        part = pl.ds(pl.multiple_of(k * depth, depth), depth)
        return pltpu.make_async_copy(cw_hbm.at[part], cw.at[part], cw_sem.at[k])

    parent_in = pltpu.make_async_copy(parent_hbm, merged, parent_sem)
    rw_in = pltpu.make_async_copy(rw_hbm, rw_ref, small_sem.at[0])
    prio_in = pltpu.make_async_copy(prio_hbm, prio_ref, small_sem.at[1])
    offs_in = pltpu.make_async_copy(offs_hbm, offs_ref, small_sem.at[2])
    rate_in = pltpu.make_async_copy(rate_hbm, rate_ref, small_sem.at[3])
    rw_in.start()
    child_in(0).start()
    for k in range(AHEAD):
        cw_in(k).start()
    offs_in.start()
    rate_in.start()
    prio_in.start()
    barrier = pltpu.get_barrier_semaphore()

    def greet_tile(d, carry):
        pl.semaphore_signal(
            barrier, inc=1, device_id={"tile": lax.rem(me_t + d, tiles)}, device_id_type=MESH
        )
        return carry

    lax.fori_loop(1, tiles, greet_tile, 0)
    for d in range(1, nests):
        there = lax.rem(me_n + d, nests)
        pl.semaphore_signal(barrier, inc=1, device_id={"nest": there}, device_id_type=MESH)
        for step in (1, tiles - 1):
            where = {"nest": there, "tile": lax.rem(me_t + step, tiles)}
            pl.semaphore_signal(barrier, inc=1, device_id=where, device_id_type=MESH)

    rw_in.wait()
    rw = rw_ref[...]
    spread_rows = lax.broadcasted_iota(jnp.int32, (per * crow, crow), 0)
    spread_cols = lax.broadcasted_iota(jnp.int32, (per * crow, crow), 1)
    spread = jnp.where(lax.rem(spread_rows, crow) == spread_cols, 1.0, 0.0).astype(BF16)
    wide_r = lax.broadcasted_iota(jnp.int32, (m, per * crow), 0)
    wide_c = lax.broadcasted_iota(jnp.int32, (m, per * crow), 1)
    diagonal = wide_r // prd == wide_c // crow
    block_rw = []
    for part in split(rw):
        line = lax.dot_general(
            part, spread, (((1,), (1,)), ((), ())), preferred_element_type=F32
        )
        line = jnp.concatenate([line] * per, axis=0)
        block_rw.append(jnp.where(diagonal, line, 0.0).astype(BF16))
    both_rw = jnp.concatenate(block_rw, axis=0)

    lane_group = lax.broadcasted_iota(jnp.int32, (prd, LANES), 1) // cols
    offs_in.wait()
    rate_in.wait()
    left, top = jnp.int32(0), jnp.int32(0)
    for n in range(nests):
        left = jnp.where(me_n == n, offs_ref[1, n], left)
        top = jnp.where(me_n == n, offs_ref[0, n], top)
    top = lax.rem(top, nrows)

    here = pl.ds(pl.multiple_of(me_t * prd, prd), prd)

    def fold(both, high, b_high, b_low):
        wide = dot(both, b_high)
        return (wide[:m] + wide[m:]) + dot(high, b_low)

    def thin(g):
        block = child[pl.ds(g * per, per)].reshape(per * crow, ccols)
        thinned = fold(both_rw, block_rw[0], *split(block))
        high, low = split(thinned)
        both_ref[:m] = high
        both_ref[m:] = low

    def cut(g):
        restricted = pltpu.roll(restricted_ref[...], left, 1)
        for base in range(0, tiles * cols, LANES):
            parts = [restricted[j * prd : (j + 1) * prd, base : base + LANES] for j in range(per)]
            step = per // 2
            while step:
                for a in range(per):
                    if a & step:
                        continue
                    one, two = parts[a], parts[a + step]
                    keep = lane_group & step == 0
                    parts[a] = jnp.where(keep, one, pltpu.roll(two, step * cols, 1))
                    parts[a + step] = jnp.where(keep, pltpu.roll(one, LANES - step * cols, 1), two)
                step //= 2
            for q in range(per):
                pieces[g, base // cols + q] = parts[q]
        strips[g, here, :] = pieces[g, me_t]

    def send(g):
        def send_one(d, carry):
            t = lax.rem(me_t + d, tiles)
            remote(
                pieces.at[g, t],
                strips.at[g, here, :],
                a2a_send.at[g],
                a2a_recv.at[g],
                {"tile": t},
            ).start()
            return carry

        lax.fori_loop(1, tiles, send_one, 0)

    def first():
        child_in(0).wait()
        cw_in(AHEAD).start()
        thin(0)
        for k in range(0, chunks, SPAN):
            part = slice(k * depth, (k + SPAN) * depth)
            for c in range(k, k + SPAN):
                cw_in(c).wait()
                if c + AHEAD + 1 < chunks:
                    cw_in(c + AHEAD + 1).start()
                for g in range(1, groups):
                    if c == min(chunks - AHEAD - 2 + g, chunks - 1):
                        child_in(g).start()
            w_high, w_low = split(cw[part])
            cw_high[part] = w_high
            cw_low[part] = w_low
            now = fold(both_ref[:, part], both_ref[:m, part], w_high, w_low)
            restricted_ref[...] = now if k == 0 else restricted_ref[...] + now
        cut(0)
        parent_in.start()
        pl.semaphore_wait(barrier, tiles - 1 + 3 * (nests - 1))
        swap_priorities()
        send(0)

    def restrict(g, carry):
        child_in(g).wait()
        thin(g)
        restricted_ref[...] = fold(both_ref[...], both_ref[:m], cw_high[...], cw_low[...])
        cut(g)
        send(g)
        return carry

    def a2a_bytes(g):
        most = strips.at[g, pl.ds(0, prd * (tiles - 1)), :]
        return remote(most, most, a2a_send.at[g], a2a_recv.at[g], {"tile": me_t})

    prio_in.wait()
    prio = prio_ref[...]
    west_t, east_t = lax.rem(me_t + tiles - 1, tiles), lax.rem(me_t + 1, tiles)
    low_n, high_n = lax.rem(me_n + nests - 1, nests), lax.rem(me_n + 1, nests)
    lane = lax.broadcasted_iota(jnp.int32, (cols, LANES), 1)

    near = lax.rem(me_n + 1, 2)
    half = LANES // 2
    halves = pl.ds(0, half), pl.ds(half, half)
    sent = {}

    def pass_on(key, source, target, sems, to, tile=None):
        where = {"nest": to} if tile is None else {"nest": to, "tile": tile}
        copy = remote(source, target, *sems, where)
        copy.start()
        sent[key] = copy

    def swap_priorities():
        for side, to in enumerate((high_n, low_n)):
            sems = near_send.at[side], near_recv.at[side]
            pass_on(("prio", side), prio_ref, prio_near.at[side], sems, to)

    strip_row = lax.broadcasted_iota(jnp.int32, (nrows, LANES), 0)

    def forward(g):
        a2a_bytes(g).wait_recv()
        turned = pltpu.roll(strips[g].T, top, 1)
        for b in range(nrows // rows):
            blocks[g, b] = turned[:, b * rows : (b + 1) * rows]
        for side, to in enumerate((high_n, low_n)):
            source = blocks.at[g, 1 - near, halves[side]]
            sems = via_send.at[g, side], via_recv.at[g, side]
            pass_on(("via", g, side), source, via.at[g, side], sems, to)
        for side, to in enumerate((high_n, low_n)):
            part = halves[1 - side]
            sems = slab_send.at[g, side], slab_recv.at[g, side]
            source = blocks.at[g, near, part]
            pass_on(("slab", g, side), source, slabs.at[g, side, part], sems, to)
        for side, col in enumerate((0, cols - 1)):
            for j in range(per):
                at = j * cols + col
                for b in range(nrows // rows):
                    ew_line[g, side, b, j : j + 1] = turned[at : at + 1, b * rows : (b + 1) * rows]
        for q, residue in enumerate((nrows - 1, rows, rows - 1, 0)):
            picked = strip_row == lax.rem(residue + nrows - top, nrows)
            line = jnp.sum(jnp.where(picked, strips[g], 0.0), axis=0, keepdims=True)
            ns_cand[g, q : q + 1] = line
            ns_cand[g, q + 4 : q + 5] = line
        for d in range(nests):
            to = lax.rem(me_n + d, nests)
            for side, tile in enumerate((west_t, east_t)):
                source = ew_line.at[g, side, lax.rem(to, 2)]
                sems = ew_send.at[g, side, d], ew_recv.at[g, side, d]
                pass_on(("ew", g, side, d), source, ew_cand.at[g, side, d], sems, to, tile)
            if d:
                source, target = ns_cand.at[g, pl.ds(0, 8)], ns_cand.at[g, pl.ds(d * 8, 8)]
                sems = ns_send.at[g, d - 1], ns_recv.at[g, d - 1]
                pass_on(("ns", g, d), source, target, sems, to)

    def relay(g):
        if g == 0:
            for side in range(2):
                sent["prio", side].wait_recv()
        for side, to in enumerate((high_n, low_n)):
            sent["via", g, side].wait_recv()
            origin = (low_n, high_n)[side]
            theirs = (prio_near[1 - side] == origin)[None]
            far = via[g, side].reshape(per // 2, cols, rows)
            own = blocks[g, near, side * half : (side + 1) * half].reshape(per // 2, cols, rows)
            relayed[g, side] = jnp.where(theirs, far, own).reshape(half, rows)
            sems = slab_send.at[g, 2 + side], slab_recv.at[g, 2 + side]
            target = slabs.at[g, side, halves[side]]
            pass_on(("slab", g, 2 + side), relayed.at[g, side], target, sems, to)

    row_lane = lax.broadcasted_iota(jnp.int32, (cols, rows), 1)

    def swap_edges():
        parent_in.wait()
        prio_f = prio.astype(F32)
        for side, row in enumerate((0, rows - 1)):
            line = jnp.zeros((cols, LANES), F32)
            for f in range(planes):
                line = jnp.where(lane == f, merged[f, :, row : row + 1], line)
            ns_out[side] = jnp.where(lane == planes, prio_f[:, row : row + 1], line)
            sems = edge_send.at[side], edge_recv.at[side]
            to = (low_n, high_n)[side]
            pass_on(("old", side), ns_out.at[side], ns_old.at[side], sems, to)
        for side, col in enumerate((0, cols - 1)):
            for f in range(planes):
                ew_out[side, f : f + 1] = merged[f, col : col + 1]
            ew_out[side, planes:] = jnp.broadcast_to(prio_f[col : col + 1], (8, rows))
            sems = edge_send.at[2 + side], edge_recv.at[2 + side]
            tile = (west_t, east_t)[side]
            pass_on(("old", 2 + side), ew_out.at[side], ew_old.at[side], sems, me_n, tile)

    def merge(g):
        if g == 0:
            for side in range(4):
                sent["old", side].wait_recv()
        origins = [lax.rem(me_n + nests - d, nests).astype(F32) for d in range(nests)]
        beside = []
        for side in range(2):
            line = ew_old[side, g * per : (g + 1) * per]
            owner = ew_old[side, planes:]
            for d in range(nests):
                sent["ew", g, side, d].wait_recv()
                line = jnp.where(owner == origins[d], ew_cand[g, side, d], line)
            beside.append(line)
        for d in range(1, nests):
            sent["ns", g, d].wait_recv()
        lines = [
            ns_cand[g, pl.ds(d * 8 + 2 * (1 - near) + way, 1), :]
            for way in range(2)
            for d in range(nests)
        ]
        lines.append(jnp.zeros((LANES - 2 * nests, LANES), F32))
        ends = jnp.concatenate(lines, axis=0).T
        outers = []
        for j in range(per):
            f = g * per + j
            outer = []
            for way in range(2):
                old = ns_old[1 - way]
                cell, owner = old[:, f : f + 1], old[:, planes : planes + 1]
                for d in range(nests):
                    at = way * nests + d
                    new = ends[j * cols : (j + 1) * cols, at : at + 1]
                    cell = jnp.where(owner == origins[d], new, cell)
                outer.append(cell)
            outers.append(outer)
        now = merged[g * per : (g + 1) * per]
        mine = blocks[g, 1 - near].reshape(per, cols, rows)
        now = jnp.where((prio == me_n)[None], mine, now)
        for q in range(4):
            sent["slab", g, q].wait_recv()
        far_n = lax.rem(me_n + 2, nests)
        ways = [(prio == n)[None] for n in (low_n, high_n)]
        far = (prio == far_n)[None]
        mixed = []
        for side in range(2):
            part = now[side * (per // 2) : (side + 1) * (per // 2)]
            for way in range(2):
                take = (ways[way] | far) if way == side else ways[way]
                slab = slabs[g, way, side * half : (side + 1) * half]
                part = jnp.where(take, slab.reshape(per // 2, cols, rows), part)
            mixed.append(part)
        now = jnp.concatenate(mixed, axis=0)
        for j in range(per):
            f = g * per + j
            here_j, outer = now[j], outers[j]
            east = jnp.concatenate([here_j[1:], beside[0][j : j + 1]], axis=0)
            west = jnp.concatenate([beside[1][j : j + 1], here_j[:-1]], axis=0)
            above = jnp.where(me_n == nests - 1, here_j[:, rows - 1 :], outer[1])
            below = jnp.where(me_n == 0, here_j[:, :1], outer[0])
            north = jnp.where(row_lane == rows - 1, above, pltpu.roll(here_j, rows - 1, 1))
            south = jnp.where(row_lane == 0, below, pltpu.roll(here_j, 1, 1))
            result[f] = here_j + rate_ref[f] * (east + west + north + south - 4.0 * here_j)

    first()
    lax.fori_loop(1, groups, restrict, 0)
    swap_edges()
    stages = {"F": forward, "P": relay, "M": merge}
    for step in order(groups):
        stages[step[0]](step[1])

    for g in range(groups):
        a2a_bytes(g).wait_send()
    for copy in sent.values():
        copy.wait_send()


def per_device(
    child_fields, row_weights, col_weights, nest_offsets, priority, parent_old, smooth_rate
):
    planes, crow, ccols = child_fields.shape[1:]
    prd = row_weights.shape[0]
    _, cols, rows = parent_old.shape
    tiles, nests = lax.axis_size("tile"), lax.axis_size("nest")
    per = LANES // cols
    groups = planes // per
    nrows = prd * tiles
    hbm = pl.BlockSpec(memory_space=pl.ANY)
    dma = pltpu.SemaphoreType.DMA
    return pl.pallas_call(
        functools.partial(kernel, tiles, nests),
        out_shape=pltpu.VMEM(parent_old.shape, F32),
        in_specs=[hbm] * 7,
        out_specs=pl.BlockSpec(memory_space=pltpu.VMEM),
        scratch_shapes=[
            pltpu.SMEM((2, nests), jnp.int32),
            pltpu.SMEM((planes,), F32),
            pltpu.VMEM(row_weights.shape, F32),
            pltpu.VMEM((cols, rows), jnp.int32),
            pltpu.VMEM((planes, crow, ccols), F32),
            pltpu.VMEM(col_weights.shape, F32),
            pltpu.VMEM(col_weights.shape, BF16),
            pltpu.VMEM(col_weights.shape, BF16),
            pltpu.VMEM((2 * per * prd, ccols), BF16),
            pltpu.VMEM((per * prd, col_weights.shape[1]), F32),
            pltpu.VMEM((planes, cols, rows), F32),
            pltpu.VMEM((groups, tiles, prd, LANES), F32),
            pltpu.VMEM((groups, nrows, LANES), F32),
            pltpu.VMEM((groups, nrows // rows, LANES, rows), F32),
            pltpu.VMEM((groups, 2, LANES // 2, rows), F32),
            pltpu.VMEM((groups, 2, LANES // 2, rows), F32),
            pltpu.VMEM((groups, 2, LANES, rows), F32),
            pltpu.VMEM((2, cols, rows), jnp.int32),
            pltpu.VMEM((2, planes + 8, rows), F32),
            pltpu.VMEM((2, planes + 8, rows), F32),
            pltpu.VMEM((2, cols, LANES), F32),
            pltpu.VMEM((2, cols, LANES), F32),
            pltpu.VMEM((groups, 2, nrows // rows, per, rows), F32),
            pltpu.VMEM((groups, 2, nests, per, rows), F32),
            pltpu.VMEM((groups, 8 * nests, LANES), F32),
            dma((4,)),
            dma((groups,)),
            dma((CHUNKS,)),
            dma,
            dma((groups,)),
            dma((groups,)),
            dma((2,)),
            dma((2,)),
            dma((groups, 2)),
            dma((groups, 2)),
            dma((groups, 4)),
            dma((groups, 4)),
            dma((4,)),
            dma((4,)),
            dma((groups, 2, nests)),
            dma((groups, 2, nests)),
            dma((groups, nests - 1)),
            dma((groups, nests - 1)),
        ],
        compiler_params=pltpu.CompilerParams(
            collective_id=0, has_side_effects=True, vmem_limit_bytes=60 * 2**20
        ),
    )(nest_offsets.T, smooth_rate, row_weights, priority, child_fields, col_weights, parent_old)


def solution(mesh):
    return jax.shard_map(
        per_device,
        mesh=mesh,
        in_specs=(
            P("nest", None, "tile", None),
            P(),
            P(),
            P(),
            P("tile", "nest"),
            P(None, "tile", "nest"),
            P(),
        ),
        out_specs=P(None, "tile", "nest"),
        check_vma=False,
    )
```
